64 devices in a mesh: rep: 8 (over x, y, core), dp: 8 (over z).
Axes of the slice: x: 2, y: 2, z: 8, core: 2. Of those that a mesh axis runs over, the one named last changes fastest.
The devices are a block of a 4x4x8 slice.
Arguments:
- x: bfloat16 [64, 4096, 512], P(('rep', 'dp')), parts along dimension 0
- dy: bfloat16 [64, 4096, 512], P(('rep', 'dp')), parts along dimension 0
- w_gate: bfloat16 [2, 512, 1536], P(None, 'dp')
- w_up: bfloat16 [2, 512, 1536], P(None, 'dp')
- w_down: bfloat16 [2, 1536, 512], P(None, 'dp')
Outputs:
- output 1: bfloat16 [64, 4096, 512], P(('rep', 'dp')), parts along dimension 0
- output 2: bfloat16 [16, 512, 1536], P('rep', 'dp'), parts along dimension 0
- output 3: bfloat16 [16, 512, 1536], P('rep', 'dp'), parts along dimension 0
- output 4: bfloat16 [16, 1536, 512], P('rep', 'dp'), parts along dimension 0
There are 8 independent parts. The reference program is written for one: setup_inputs(seed, part) draws one part's arguments, and reference() takes and returns one part's arrays. A program takes and returns all parts, laid end to end along the dimension named above; an argument that names none is the same for every part.
All inputs are finite; a program needn't handle non-finite values.
Results may differ from the reference program's by a relative error of at most 0.018.
Values are sent between devices in bfloat16 or wider.
A program may use at most 768 MiB of HBM per device.

```python
import jax
import jax.numpy as jnp
from jax import lax

SEQUENCES = 8
TOKENS = 4096
D = 512
FF = 1536
LAYERS = 2
NAMES = ("w_gate", "w_up", "w_down")
SHAPES = {"w_gate": (LAYERS, D, FF), "w_up": (LAYERS, D, FF), "w_down": (LAYERS, FF, D)}


def bump(key, n, height):
    away = (jnp.arange(n, dtype=jnp.int32) - jax.random.randint(key, (), 0, n, jnp.int32)) % n
    return jnp.where(away < n // 8, height, 1.0)


def together(key, own, strength):
    shared = jax.random.normal(key, own.shape[1:], jnp.float32)
    return (own + strength * shared) * lax.rsqrt(1 + strength * strength)


def setup_inputs(seed: int = 0, part: int = 0) -> dict:
    kx, kdy, ka, kb, kz, kf, kh, kl, *kw = jax.random.split(jax.random.key(seed), 8 + len(NAMES))
    kx, kdy, ka, kb = (jax.random.fold_in(k, part) for k in (kx, kdy, ka, kb))
    shape = (SEQUENCES, TOKENS, D)
    much_x, much_dy = jax.random.uniform(kz, (2,), jnp.float32, 0.0, 1.0)
    layers = 2.0 ** jax.random.uniform(kl, (LAYERS, 1, 1), jnp.float32, -1.0, 1.0)
    x = together(ka, jax.random.normal(kx, shape, jnp.float32), much_x) * bump(kf, D, 4.0)
    dy = together(kb, jax.random.normal(kdy, shape, jnp.float32), much_dy)
    drawn = {"x": x.astype(jnp.bfloat16), "dy": (dy * (SEQUENCES * TOKENS) ** -0.5).astype(jnp.bfloat16)}
    for key, name in zip(kw, NAMES, strict=True):
        w = jax.random.normal(key, SHAPES[name], jnp.float32) * SHAPES[name][1] ** -0.5
        drawn[name] = (w * {"w_gate": 1.0, "w_up": bump(kh, FF, 4.0), "w_down": layers}[name]).astype(jnp.bfloat16)
    return drawn


def matmul(a, w):
    return jnp.dot(a, w, preferred_element_type=jnp.float32).astype(jnp.bfloat16)


def normed(h):
    wide = h.astype(jnp.float32)
    scale = lax.rsqrt(jnp.mean(wide**2, -1, keepdims=True) + 1e-6)
    return (wide * scale).astype(jnp.bfloat16)


def layer(h, w):
    a = normed(h)
    gate = jnp.dot(a, w["w_gate"], preferred_element_type=jnp.float32)
    up = jnp.dot(a, w["w_up"], preferred_element_type=jnp.float32)
    return h + matmul((jax.nn.silu(gate) * up).astype(jnp.bfloat16), w["w_down"])


def stack(weights, h):
    return lax.scan(lambda h, w: (layer(h, w), None), h, weights)[0]


def reference(x, dy, w_gate, w_up, w_down):
    weights = dict(zip(NAMES, (w_gate, w_up, w_down), strict=True))

    def take(so_far, sequence):
        h, by_y = sequence
        _, back = jax.vjp(stack, weights, h)
        by_weights, by_h = back(by_y)
        return jax.tree.map(lambda total, term: total + term.astype(jnp.float32), so_far, by_weights), by_h

    none_yet = {name: jnp.zeros(w.shape, jnp.float32) for name, w in weights.items()}
    by_weights, by_x = lax.scan(take, none_yet, (x, dy))
    return (by_x, *(by_weights[name].astype(jnp.bfloat16) for name in NAMES))
```

```python
import functools

import jax
import jax.numpy as jnp
from jax import lax
from jax.experimental import pallas as pl
from jax.experimental.pallas import tpu as pltpu
from jax.sharding import PartitionSpec as P

BF = jnp.bfloat16
F32 = jnp.float32
CHUNKS = 3
TM = 256
EPS = 1e-6
VMEM_LIMIT = 67043328


def dot(a, b):
    return lax.dot_general(a, b, (((1,), (0,)), ((), ())), preferred_element_type=F32)


def dot_nt(a, b):
    return lax.dot_general(a, b, (((1,), (1,)), ((), ())), preferred_element_type=F32)


def dot_tn(a, b):
    return lax.dot_general(a, b, (((0,), (0,)), ((), ())), preferred_element_type=F32)


def sigmoid(g):
    return 0.5 * jnp.tanh(0.5 * g) + 0.5


def scale_of(wide):
    return lax.rsqrt(jnp.mean(wide * wide, -1, keepdims=True) + EPS)


def normed(wide):
    return (wide * scale_of(wide)).astype(BF)


def aligned(start, size):
    return pl.ds(pl.multiple_of(start, size), size)


def kernel(x_hbm, dy_hbm, w_hbm, dx_hbm, terms_hbm, h_hbm, a, y, g, w, acc, act0, act1, g0, g1, terms, io, sem, io_sem):
    layers, chunks = w.shape[:2]
    tokens, d = y.shape
    fc = w.shape[-1]
    half = fc // 2
    nt = tokens // TM
    big = io.shape[1]
    acts, gs = (act0, act1), (g0, g1)

    loads = [pltpu.make_async_copy(x_hbm, a.at[0], sem.at[0]), pltpu.make_async_copy(dy_hbm, y, sem.at[1]), pltpu.make_async_copy(w_hbm, w, sem.at[2])]
    for copy in loads:
        copy.start()
    loads[0].wait()

    def norm_x(t, _):
        rows = aligned(t * TM, TM)
        a[0, rows, :] = normed(a[0, rows, :].astype(F32))
        return 0

    lax.fori_loop(0, nt, norm_x, 0)
    loads[2].wait()

    def hidden(j, _):
        c, t = j // (nt // 4), j % (nt // 4)
        for k in range(4):
            rows = aligned((4 * t + k) * TM, TM)
            at = a[0, rows, :]
            for f in (0, half):
                gate = dot(at, w[0, c, 0, :, f : f + half])
                up = dot(at, w[0, c, 1, :, f : f + half])
                g[c, rows, f : f + half] = (gate * sigmoid(gate) * up).astype(BF)
        return 0

    lax.fori_loop(0, chunks * nt // 4, hidden, 0)

    steps = tokens // big

    def io_in(src, j):
        return pltpu.make_async_copy(src.at[aligned(j * big, big), :], io.at[j % 2], io_sem.at[0, j % 2])

    def io_out(j):
        return pltpu.make_async_copy(io.at[j % 2], h_hbm.at[aligned(j * big, big), :], io_sem.at[1, j % 2])

    io_in(x_hbm, 0).start()

    def down(j, _):
        io_in(x_hbm, j).wait()

        @pl.when(j >= 1)
        def _():
            io_out(j - 1).wait()

        @pl.when(j + 1 < steps)
        def _():
            io_in(x_hbm, j + 1).start()

        for k in range(big // TM):
            rows = aligned(j * big + k * TM, TM)
            out = sum(dot(g[c, rows, :fc], w[0, c, 2]) for c in range(chunks))
            here = pl.ds(k * TM, TM)
            h = (io[j % 2, here, :].astype(F32) + out.astype(BF).astype(F32)).astype(BF)
            io[j % 2, here, :] = h
            a[1, rows, :] = normed(h.astype(F32))
        io_out(j).start()
        return 0

    lax.fori_loop(0, steps, down, 0)
    io_out(steps - 1).wait()
    loads[1].wait()

    for l in range(layers):
        for m in range(3):
            acc[m] = jnp.zeros_like(acc[m])

    def backward(turn, _):
        l = layers - 1 - turn

        def grads_in(i, slot, f):
            c, t = i // nt, i % nt
            rows = aligned(t * TM, TM)
            at, dt = a[l, rows, :], y[rows, :]
            gate = dot(at, w[l, c, 0, :, f : f + half])
            up = dot(at, w[l, c, 1, :, f : f + half])
            dact = dot_nt(dt, w[l, c, 2, f : f + half, :]).astype(BF).astype(F32)
            s = sigmoid(gate)
            silu = gate * s
            acts[slot][:, f : f + half] = (silu * up).astype(BF)
            dgate = (dact * up * (s + silu * (1.0 - s))).astype(BF)
            dup = (dact * silu).astype(BF)
            gs[slot][:, f : f + half] = dgate
            gs[slot][:, fc + f : fc + f + half] = dup
            g[c, rows, f : f + half] = dgate
            g[c, rows, fc + f : fc + f + half] = dup

        def down_grad(i, slot):
            rows = aligned(i % nt * TM, TM)
            acc[2] += dot_tn(acts[slot][...], y[rows, :])

        def in_grads(i, slot):
            rows = aligned(i % nt * TM, TM)
            at = a[l, rows, :]
            acc[0] += dot_tn(at, gs[slot][:, :fc])
            acc[1] += dot_tn(at, gs[slot][:, fc:])

        for f in (0, half):
            grads_in(0, 0, f)

        def chunk(c, _):
            def body(j, _):
                for k in range(4):
                    i = 4 * j + k
                    later = jnp.minimum(i + 1, chunks * nt - 1)
                    grads_in(later, (k + 1) % 2, 0)
                    down_grad(i, k % 2)
                    grads_in(later, (k + 1) % 2, half)
                    in_grads(i, k % 2)
                return 0

            lax.fori_loop(c * nt // 4, (c + 1) * nt // 4, body, 0)
            for m in range(3):
                terms[c, m] = acc[m].astype(BF)
                acc[m] = jnp.zeros_like(acc[m])
            return 0

        lax.fori_loop(0, chunks, chunk, 0)

        out = pltpu.make_async_copy(terms, terms_hbm.at[l], sem.at[3])
        out.start()

        def fetch(j):
            @pl.when(l == 0)
            def _():
                io_in(x_hbm, j).start()

            @pl.when(l != 0)
            def _():
                io_in(h_hbm, j).start()

        def dx_out(j):
            rows = aligned(j * big, big)
            return pltpu.make_async_copy(y.at[rows, :], dx_hbm.at[rows, :], io_sem.at[1, j % 2])

        fetch(0)

        def inputs(j, _):
            io_in(x_hbm, j).wait()

            @pl.when(j + 1 < steps)
            def _():
                fetch(j + 1)

            for k in range(big // TM):
                rows = aligned(j * big + k * TM, TM)
                da = sum(dot_nt(g[c, rows, m * fc : (m + 1) * fc], w[l, c, m]) for c in range(chunks) for m in range(2))
                da = da.astype(BF).astype(F32)
                wide = io[j % 2, pl.ds(k * TM, TM), :].astype(F32)
                scale = scale_of(wide)
                along = jnp.mean(da * wide, -1, keepdims=True) * (scale * scale * scale)
                dh = (da * scale - wide * along).astype(BF).astype(F32)
                y[rows, :] = (y[rows, :].astype(F32) + dh).astype(BF)

            @pl.when(l == 0)
            def _():
                dx_out(j).start()

            return 0

        lax.fori_loop(0, steps, inputs, 0)
        out.wait()

        @pl.when(l == 0)
        def _():
            for j in range(steps):
                dx_out(j).wait()

        return 0

    lax.fori_loop(0, layers, backward, 0)


def layers_of(x, dy, w):
    tokens, d = x.shape
    layers, chunks, _, _, fc = w.shape
    big = 4 * TM
    hbm = pl.BlockSpec(memory_space=pl.ANY)
    return pl.pallas_call(
        kernel,
        out_shape=(
            jax.ShapeDtypeStruct(x.shape, BF),
            jax.ShapeDtypeStruct(w.shape, BF),
            jax.ShapeDtypeStruct(x.shape, BF),
        ),
        in_specs=[hbm] * 3,
        out_specs=[hbm] * 3,
        scratch_shapes=[
            pltpu.VMEM((layers, tokens, d), BF),
            pltpu.VMEM((tokens, d), BF),
            pltpu.VMEM((chunks, tokens, 2 * fc), BF),
            pltpu.VMEM(w.shape, BF),
            pltpu.VMEM((3, d, fc), F32),
            pltpu.VMEM((TM, fc), BF),
            pltpu.VMEM((TM, fc), BF),
            pltpu.VMEM((TM, 2 * fc), BF),
            pltpu.VMEM((TM, 2 * fc), BF),
            pltpu.VMEM(w.shape[1:], BF),
            pltpu.VMEM((2, big, d), BF),
            pltpu.SemaphoreType.DMA((4,)),
            pltpu.SemaphoreType.DMA((2, 2)),
        ],
        compiler_params=pltpu.CompilerParams(vmem_limit_bytes=VMEM_LIMIT, has_side_effects=True),
        name="layers",
    )(x, dy, w)


def solution(mesh):
    n = mesh.shape["dp"]

    def local(x, dy, gate, up, down):
        layers, rows, ff = gate.shape
        d = x.shape[-1]
        own = ff // n // CHUNKS

        def columns(t):
            t = lax.all_gather(t, "dp", axis=1, tiled=True)
            t = t.reshape(layers, d, n, CHUNKS, own)
            return t.transpose(0, 3, 1, 2, 4).reshape(layers, CHUNKS, d, n * own)

        def rows_of(t):
            t = lax.all_gather(t, "dp", axis=1, tiled=True)
            t = t.reshape(layers, n, CHUNKS, own, d)
            return t.transpose(0, 2, 1, 3, 4).reshape(layers, CHUNKS, n * own, d)

        w = jnp.stack([columns(gate), columns(up), rows_of(down)], 2)
        dx, terms, _ = layers_of(x[0], dy[0], w)

        def back_columns(t):
            t = t.reshape(layers, CHUNKS, d, n, own).transpose(0, 2, 3, 1, 4).reshape(layers, d, ff)
            return lax.psum_scatter(t, "dp", scatter_dimension=1, tiled=True)

        def back_rows(t):
            t = t.reshape(layers, CHUNKS, n, own, d).transpose(0, 2, 1, 3, 4).reshape(layers, ff, d)
            return lax.psum_scatter(t, "dp", scatter_dimension=1, tiled=True)

        return dx[None], back_columns(terms[:, :, 0]), back_columns(terms[:, :, 1]), back_rows(terms[:, :, 2])

    both, rows = P(("rep", "dp"), None, None), P(None, "dp", None)
    return jax.shard_map(
        local, mesh=mesh, in_specs=(both, both, rows, rows, rows),
        out_specs=(both, P("rep", "dp", None), P("rep", "dp", None), P("rep", "dp", None)), check_vma=False,
    )
```

```python
import functools

import jax
import jax.numpy as jnp
from jax import lax
from jax.experimental import pallas as pl
from jax.experimental.pallas import tpu as pltpu
from jax.sharding import PartitionSpec as P

BF = jnp.bfloat16
F32 = jnp.float32
CHUNKS = 3
TILES = 16
EPS = 1e-6
VMEM_LIMIT = 67043328


def dot(a, b):
    return lax.dot_general(a, b, (((1,), (0,)), ((), ())), preferred_element_type=F32)


def dot_nt(a, b):
    return lax.dot_general(a, b, (((1,), (1,)), ((), ())), preferred_element_type=F32)


def dot_tn(a, b):
    return lax.dot_general(a, b, (((0,), (0,)), ((), ())), preferred_element_type=F32)


def sigmoid(g):
    return 0.5 * jnp.tanh(0.5 * g) + 0.5


def scale_of(wide):
    return lax.rsqrt(jnp.mean(wide * wide, -1, keepdims=True) + EPS)


def normed(wide):
    return (wide * scale_of(wide)).astype(BF)


def aligned(start, size):
    return pl.ds(pl.multiple_of(start, size), size)


def kernel(
    n, x_hbm, dy_hbm, gate_hbm, up_hbm, down_hbm, dx_hbm, dgate_hbm, dup_hbm, ddown_hbm, h_hbm,
    a, y, g, w, acc, act0, act1, g0, g1, terms, slots, fin, fixed, io,
    sem, io_sem, out_sem, ag_recv, ag_send, side_recv, rs_recv, rs_send, credit,
):
    layers, chunks = w.shape[:2]
    tokens, d = y.shape
    fc = w.shape[-1]
    own = d // n
    half = fc // 2
    tm = tokens // TILES
    big = 2 * tm
    per = TILES // 2
    acts, gs = (act0, act1), (g0, g1)
    near = (n - 1) // 2
    items = layers * chunks * 3

    me = lax.axis_index("dp")
    core = lax.axis_index("rep") % 2
    left, right = {"dp": (me + n - 1) % n}, {"dp": (me + 1) % n}
    partner = {"rep": lax.axis_index("rep") + 1 - 2 * core}

    def place(c, m, s):
        return s + jnp.where((m == 2) & (c == 1), 1 - 2 * (s % 2), 0)

    def remote(src, dst, send, recv, to):
        return pltpu.make_async_remote_copy(src, dst, send, recv, device_id=to, device_id_type=pl.DeviceIdType.MESH)

    def item(i):
        l, r = i // (chunks * 3), i % (chunks * 3)
        first = l == 0
        c = jnp.where(first, jnp.where(r < 2 * chunks, r // 2, r - 2 * chunks), r // 3)
        m = jnp.where(first, jnp.where(r < 2 * chunks, r % 2, 2), r % 3)
        return l, c, m

    def gather(k):
        def hop(back, _):
            h = near + 1 - back
            i = k - 2 * h

            @pl.when((i >= 0) & (i < items))
            def _():
                l, c, m = item(i)
                far = near + i % 2

                def way(side, _):
                    reach = jnp.where(side == 0, far, n - 1 - far)
                    s = jnp.where(side == 0, me + n - h, me + h) % n
                    rows = aligned(place(c, m, s) * own + core * (own // 2), own // 2)
                    ref = w.at[l, c, m, rows, :]
                    at = jnp.where(side == 0, 0, far) + h
                    to = {"dp": jnp.where(side == 0, me + 1, me + n - 1) % n}

                    @pl.when((h >= 1) & (h <= reach))
                    def _():
                        remote(ref, ref, ag_send.at[i], ag_recv.at[i, at - 1], to).wait_recv()

                    @pl.when(h < reach)
                    def _():
                        remote(ref, ref, ag_send.at[i], ag_recv.at[i, at], to).start()

                    @pl.when((h >= 1) & (h <= reach))
                    def _():
                        remote(ref, ref, ag_send.at[i], side_recv.at[i], partner).start()

                    return 0

                lax.fori_loop(0, 2, way, 0)

            return 0

        lax.fori_loop(0, near + 2, hop, 0)

    def arrived(i):
        l, c, m = item(i)
        ref = w.at[l, c, m, pl.ds(0, (n - 1) * (own // 2)), :]
        pltpu.make_async_copy(ref, ref, side_recv.at[i]).wait()

    def reduce(turn, q):
        late = q >= per

        def unit(u, _):
            base = jnp.where(late, q - per - u, q + 3 * per - u)
            t = jnp.where(late, turn, turn - 1)
            p = (2 * (base + 3)) % 3
            since = base - per * p
            s = since // 3

            @pl.when((t >= 0) & (since >= 0) & (since <= 3 * (near + 1)))
            def _():
                far = near + (p + u) % 2

                def way(side, _):
                    reach = jnp.where(side == 0, far, n - 1 - far)
                    at = jnp.where(side == 0, 0, far) + s
                    to = {"dp": jnp.where(side == 0, me + 1, me + n - 1) % n}
                    o = jnp.where(side == 0, me + reach - s, me + n - reach + s) % n
                    rows = aligned(place(p, u, o) * own, own)

                    @pl.when((s == 0) & (t >= 1))
                    def _():
                        pl.semaphore_wait(credit.at[side, p, u], 1)

                    @pl.when(s == 0)
                    def _():
                        remote(terms.at[p, u, rows, :], slots.at[p, u, at], rs_send.at[p, u], rs_recv.at[p, u, at], to).start()

                    @pl.when((s >= 1) & (s < reach))
                    def _():
                        ref = slots.at[p, u, at - 1]
                        remote(ref, ref, rs_send.at[p, u], rs_recv.at[p, u, at - 1], to).wait_recv()
                        ref[...] = (ref[...].astype(F32) + terms[p, u, rows, :].astype(F32)).astype(BF)
                        remote(ref, slots.at[p, u, at], rs_send.at[p, u], rs_recv.at[p, u, at], to).start()

                    return 0

                lax.fori_loop(0, 2, way, 0)

                @pl.when(s == near + 1)
                def _():
                    finish(t, p, u, far)

            return 0

        lax.fori_loop(0, 3, unit, 0)

    def down_out(l, p):
        return pltpu.make_async_copy(fin.at[p, 2], ddown_hbm.at[l, aligned(p * own, own), :], out_sem.at[p])

    def in_out(l, m, j):
        out = dgate_hbm if m == 0 else dup_hbm
        return pltpu.make_async_copy(fixed.at[m, j], out.at[l, :, pl.ds(j * d, d)], out_sem.at[chunks + m * chunks + j])

    def finish(t, p, u, far):
        l = layers - 1 - t
        ends = [slots.at[p, u, far - 1], slots.at[p, u, n - 2]]
        for ref, at in zip(ends, (far - 1, n - 2)):
            remote(ref, ref, rs_send.at[p, u], rs_recv.at[p, u, at], right).wait_recv()

        @pl.when((t >= 1) & (u == 2))
        def _():
            down_out(l, p).wait()

        rows = aligned(place(p, u, me) * own, own)
        fin[p, u] = (ends[0][...].astype(F32) + ends[1][...].astype(F32) + terms[p, u, rows, :].astype(F32)).astype(BF)
        ref = w.at[0, 0, 0, pl.ds(0, (n - 1) * own), :]
        pltpu.make_async_copy(ref, ref, rs_send.at[p, u]).wait()

        @pl.when(t < layers - 1)
        def _():
            pl.semaphore_signal(credit.at[0, p, u], 1, device_id=left, device_id_type=pl.DeviceIdType.MESH)
            pl.semaphore_signal(credit.at[1, p, u], 1, device_id=right, device_id_type=pl.DeviceIdType.MESH)

        @pl.when(u == 2)
        def _():
            down_out(l, p).start()

        @pl.when((u == 2) & (p == chunks - 1))
        def _():
            outs = [in_out(l, m, j) for m in range(2) for j in range(3)]

            @pl.when(t >= 1)
            def _():
                for copy in outs:
                    copy.wait()

            low = lax.broadcasted_iota(jnp.int32, (own, 128), 1) < 64
            for m in range(2):
                for e in range(fc // 128):
                    c0, c1, c2 = (fin[c, m, :, pl.ds(128 * e, 128)].astype(F32) for c in range(chunks))
                    for k, (lo, hi) in enumerate(((c0, c1), (c2, c0), (c1, c2))):
                        j, at = divmod(3 * e + k, d // 128)
                        fixed[m, j, :, pl.ds(128 * at, 128)] = jnp.where(low, lo, hi).astype(BF)
            for copy in outs:
                copy.start()

    shards = (gate_hbm, up_hbm)
    raw = [
        pltpu.make_async_copy(shards[m].at[l, :, pl.ds(j * d, d)], terms.at[l, m, pl.ds(j * own, own), :], sem.at[2 + (l * 2 + m) * 3 + j])
        for l in range(layers) for m in range(2) for j in range(3)
    ]
    downs = [
        pltpu.make_async_copy(down_hbm.at[l, pl.ds(c * own, own), :], w.at[l, c, 2, aligned(place(c, 2, me) * own, own), :], sem.at[2 + layers * 6 + l * 3 + c])
        for l in range(layers) for c in range(chunks)
    ]
    load_x, load_dy = pltpu.make_async_copy(x_hbm, a.at[0], sem.at[0]), pltpu.make_async_copy(dy_hbm, y, sem.at[1])
    for copy in (*raw, *downs, load_x, load_dy):
        copy.start()
    barrier = pltpu.get_barrier_semaphore()
    for to in (left, right, partner):
        pl.semaphore_signal(barrier, 1, device_id=to, device_id_type=pl.DeviceIdType.MESH)
    for copy in (*raw, *downs):
        copy.wait()
    low = lax.broadcasted_iota(jnp.int32, (own, 128), 1) < 64
    mine = aligned(me * own, own)
    for l in range(layers):
        for m in range(2):
            for e in range(fc // 128):
                parts = []
                for k in range(3):
                    j, at = divmod(3 * e + k, d // 128)
                    parts.append(terms[l, m, pl.ds(j * own, own), pl.ds(128 * at, 128)].astype(F32))
                k0, k1, k2 = parts
                for c, (lo, hi) in enumerate(((k0, k1), (k2, k0), (k1, k2))):
                    w[l, c, m, mine, pl.ds(128 * e, 128)] = jnp.where(low, lo, hi).astype(BF)
    pl.semaphore_wait(barrier, 3)

    def gather_some(k, _):
        gather(k)
        return 0

    lax.fori_loop(0, 2, gather_some, 0)
    load_x.wait()

    def norm_x(t, _):
        rows = aligned(t * tm, tm)
        a[0, rows, :] = normed(a[0, rows, :].astype(F32))
        return 0

    lax.fori_loop(0, TILES, norm_x, 0)
    done = 2 * (near + 1)
    lax.fori_loop(2, done + 2, gather_some, 0)

    bodies = TILES // 4

    def hidden(j, _):
        c, t = j // bodies, j % bodies

        @pl.when(j % 2 == 1)
        def _():
            gather(done + 2 + j // 2)

        @pl.when(t == 0)
        def _():
            arrived(2 * c)
            arrived(2 * c + 1)

        for k in range(4):
            rows = aligned((4 * t + k) * tm, tm)
            at = a[0, rows, :]
            for f in (0, half):
                gate = dot(at, w[0, c, 0, :, f : f + half])
                up = dot(at, w[0, c, 1, :, f : f + half])
                g[c, rows, f : f + half] = (gate * sigmoid(gate) * up).astype(BF)
        return 0

    lax.fori_loop(0, chunks * bodies, hidden, 0)

    def io_in(src, j):
        return pltpu.make_async_copy(src.at[aligned(j * big, big), :], io.at[j % 2], io_sem.at[0, j % 2])

    def io_out(j):
        return pltpu.make_async_copy(io.at[j % 2], h_hbm.at[aligned(j * big, big), :], io_sem.at[1, j % 2])

    later = done + 2 + chunks * bodies // 2
    io_in(x_hbm, 0).start()
    gather(later)
    for c in range(chunks):
        arrived(2 * chunks + c)

    def down(j, _):
        @pl.when((j % 2 == 0) & (j >= 2))
        def _():
            gather(later + j // 2)

        io_in(x_hbm, j).wait()

        @pl.when(j >= 1)
        def _():
            io_out(j - 1).wait()

        @pl.when(j + 1 < per)
        def _():
            io_in(x_hbm, j + 1).start()

        for k in range(2):
            rows = aligned(j * big + k * tm, tm)
            out = sum(dot(g[c, rows, :fc], w[0, c, 2]) for c in range(chunks))
            here = pl.ds(k * tm, tm)
            h = (io[j % 2, here, :].astype(F32) + out.astype(BF).astype(F32)).astype(BF)
            io[j % 2, here, :] = h
            a[1, rows, :] = normed(h.astype(F32))
        io_out(j).start()
        return 0

    lax.fori_loop(0, per, down, 0)
    last = later + per // 2
    io_out(per - 1).wait()
    load_dy.wait()

    for m in range(3):
        acc[m] = jnp.zeros_like(acc[m])

    def backward(turn, _):
        l = layers - 1 - turn

        def grads_in(i, slot, f):
            c, t = i // TILES, i % TILES
            rows = aligned(t * tm, tm)
            at, dt = a[l, rows, :], y[rows, :]
            gate = dot(at, w[l, c, 0, :, f : f + half])
            up = dot(at, w[l, c, 1, :, f : f + half])
            dact = dot_nt(dt, w[l, c, 2, f : f + half, :]).astype(BF).astype(F32)
            s = sigmoid(gate)
            silu = gate * s
            acts[slot][:, f : f + half] = (silu * up).astype(BF)
            dgate = (dact * up * (s + silu * (1.0 - s))).astype(BF)
            dup = (dact * silu).astype(BF)
            gs[slot][:, f : f + half] = dgate
            gs[slot][:, fc + f : fc + f + half] = dup
            g[c, rows, f : f + half] = dgate
            g[c, rows, fc + f : fc + f + half] = dup

        def down_grad(i, slot):
            rows = aligned(i % TILES * tm, tm)
            acc[2] += dot_tn(acts[slot][...], y[rows, :])

        def in_grads(i, slot):
            rows = aligned(i % TILES * tm, tm)
            at = a[l, rows, :]
            acc[0] += dot_tn(at, gs[slot][:, :fc])
            acc[1] += dot_tn(at, gs[slot][:, fc:])

        @pl.when(turn == 0)
        def _():
            for m in range(3):
                arrived(items // layers * (layers - 1) + m)

        for f in (0, half):
            grads_in(0, 0, f)

        def body(j, _):
            @pl.when((turn == 0) & (last + j < items + done))
            def _():
                gather(last + j)

            @pl.when((turn == 0) & (j % per == per - 1) & (j < (chunks - 1) * per))
            def _():
                for m in range(3):
                    arrived(items // layers * (layers - 1) + 3 * (j // per + 1) + m)

            reduce(turn, j)
            for k in range(2):
                i = 2 * j + k
                ahead = jnp.minimum(i + 1, chunks * TILES - 1)
                grads_in(ahead, (k + 1) % 2, 0)
                down_grad(i, k % 2)
                grads_in(ahead, (k + 1) % 2, half)
                in_grads(i, k % 2)
            return 0

        def chunk(c, _):
            lax.fori_loop(c * per, (c + 1) * per, body, 0)
            for m in range(3):
                terms[c, m] = acc[m].astype(BF)
                acc[m] = jnp.zeros_like(acc[m])
            return 0

        lax.fori_loop(0, chunks, chunk, 0)

        def fetch(j):
            @pl.when(l == 0)
            def _():
                io_in(x_hbm, j).start()

            @pl.when(l != 0)
            def _():
                io_in(h_hbm, j).start()

        fetch(0)

        def inputs(j, _):
            reduce(turn, chunks * per + j)
            io_in(x_hbm, j).wait()

            @pl.when(j + 1 < per)
            def _():
                fetch(j + 1)

            for k in range(2):
                rows = aligned(j * big + k * tm, tm)
                da = sum(dot_nt(g[c, rows, m * fc : (m + 1) * fc], w[l, c, m]) for c in range(chunks) for m in range(2))
                da = da.astype(BF).astype(F32)
                wide = io[j % 2, pl.ds(k * tm, tm), :].astype(F32)
                scale = scale_of(wide)
                along = jnp.mean(da * wide, -1, keepdims=True) * (scale * scale * scale)
                dh = (da * scale - wide * along).astype(BF).astype(F32)
                y[rows, :] = (y[rows, :].astype(F32) + dh).astype(BF)

            @pl.when(l == 0)
            def _():
                rows = aligned(j * big, big)
                pltpu.make_async_copy(y.at[rows, :], dx_hbm.at[rows, :], sem.at[0]).start()

            return 0

        lax.fori_loop(0, per, inputs, 0)
        return 0

    lax.fori_loop(0, layers, backward, 0)

    def tail(q, _):
        reduce(layers - 1, q)
        return 0

    lax.fori_loop((chunks + 1) * per, (chunks + 1) * per + 3 * (near + 1) + 3 - per, tail, 0)
    for p in range(chunks):
        down_out(0, p).wait()
    for m in range(2):
        for j in range(3):
            in_out(0, m, j).wait()
    pltpu.make_async_copy(y, dx_hbm, sem.at[0]).wait()

    def sent(i, _):
        ref = w.at[0, 0, 0, pl.ds(0, (n - 1) * own), :]
        pltpu.make_async_copy(ref, ref, ag_send.at[i]).wait()
        return 0

    lax.fori_loop(0, items, sent, 0)


def layers_of(n, x, dy, gate, up, down):
    tokens, d = x.shape
    layers, own, ff = gate.shape
    fc = ff // CHUNKS
    tm = tokens // TILES
    items = layers * CHUNKS * 3
    assert d == fc == n * own and down.shape == (layers, CHUNKS * own, d) and own == 64 and n % 2 == 0
    assert (TILES // 2) % 3 == 2 and layers > 1
    hbm = pl.BlockSpec(memory_space=pl.ANY)
    dma = pltpu.SemaphoreType.DMA
    near = (n - 1) // 2
    return pl.pallas_call(
        functools.partial(kernel, n),
        out_shape=[jax.ShapeDtypeStruct(t.shape, BF) for t in (x, gate, up, down, x)],
        in_specs=[hbm] * 5,
        out_specs=[hbm] * 5,
        scratch_shapes=[
            pltpu.VMEM((layers, tokens, d), BF),
            pltpu.VMEM((tokens, d), BF),
            pltpu.VMEM((CHUNKS, tokens, 2 * fc), BF),
            pltpu.VMEM((layers, CHUNKS, 3, d, fc), BF),
            pltpu.VMEM((3, d, fc), F32),
            pltpu.VMEM((tm, fc), BF),
            pltpu.VMEM((tm, fc), BF),
            pltpu.VMEM((tm, 2 * fc), BF),
            pltpu.VMEM((tm, 2 * fc), BF),
            pltpu.VMEM((CHUNKS, 3, d, fc), BF),
            pltpu.VMEM((CHUNKS, 3, n - 1, own, fc), BF),
            pltpu.VMEM((CHUNKS, 3, own, fc), BF),
            pltpu.VMEM((2, CHUNKS, own, fc), BF),
            pltpu.VMEM((2, 2 * tm, d), BF),
            dma((2 + layers * 9,)),
            dma((2, 2)),
            dma((CHUNKS * 3,)),
            dma((items, n - 1)),
            dma((items,)),
            dma((items,)),
            dma((CHUNKS, 3, n - 1)),
            dma((CHUNKS, 3)),
            pltpu.SemaphoreType.REGULAR((2, CHUNKS, 3)),
        ],
        compiler_params=pltpu.CompilerParams(vmem_limit_bytes=VMEM_LIMIT, has_side_effects=True, collective_id=0),
        name="layers",
    )(x, dy, gate, up, down)


def solution(mesh):
    n = mesh.shape["dp"]
    assert mesh.shape["rep"] % 2 == 0

    def local(x, dy, gate, up, down):
        dx, dgate, dup, ddown, _ = layers_of(n, x[0], dy[0], gate, up, down)
        return dx[None], dgate, dup, ddown

    both, rows = P(("rep", "dp"), None, None), P(None, "dp", None)
    grads = P("rep", "dp", None)
    return jax.shard_map(
        local, mesh=mesh, in_specs=(both, both, rows, rows, rows), out_specs=(both, grads, grads, grads), check_vma=False
    )
```

```python
import functools

import jax
import jax.numpy as jnp
from jax import lax
from jax.experimental import pallas as pl
from jax.experimental.pallas import tpu as pltpu
from jax.sharding import PartitionSpec as P

BF = jnp.bfloat16
F32 = jnp.float32
CHUNKS = 3
TILES = 16
BODIES = TILES // 2

GATHER_START = (
    ((0, 0), (1, 0)),
    ((0, 1), (1, 1), (2, 0), (3, 0)),
    ((0, 2), (1, 2), (2, 1), (3, 1)),
    ((0, 3), (1, 3), (2, 2), (3, 2), (4, 0), (5, 0)),
    ((0, 4), (1, 4), (2, 3), (3, 3)),
)
GATHER_HIDDEN = {
    1: ((2, 4), (3, 4), (4, 1), (5, 1), (6, 0)),
    5: ((4, 2), (5, 2)),
    9: ((4, 3), (5, 3), (6, 1)),
    13: ((4, 4), (5, 4), (7, 0)),
    14: ((6, 2),),
    18: ((6, 3), (7, 1)),
}
GATHER_DOWN = {0: ((6, 4), (7, 2)), 3: ((7, 3), (8, 0)), 6: ((7, 4),)}
GATHER_BACK = {0: ((8, 1),), 1: ((9, 0),), 2: ((8, 2),), 3: ((9, 1),), 4: ((8, 3),), 5: ((9, 2),), 6: ((8, 4),), 7: ((9, 3),), 9: ((9, 4),)}

SUMS_FIRST = [(BODIES * (p + 1) + 3 * s + u, p, u, s) for p in range(3) for s in range(5) for u in range(3)]
LATE = 4 * BODIES
SUMS_LEFT = [(1 + 4 * (s - 3) + u, 2, u, s) for s in (3, 4) for u in range(3)]
SUMS_SECOND = (
    [(8 + 4 * s + u, 0, u, s) for s in range(5) for u in range(3)]
    + [(17 + 4 * s + u, 1, u, s) for s in range(2) for u in range(3)]
    + [(25 + u, 1, u, 2) for u in range(3)] + [(28 + u, 1, u, 3) for u in range(3)] + [(31, 1, 0, 4), (31, 1, 1, 4), (32, 1, 2, 4)]
    + [(24, 2, 0, 0), (24, 2, 1, 0), (25, 2, 2, 0)] + [(27 + u, 2, u, 1) for u in range(3)] + [(30, 2, 0, 2), (31, 2, 1, 2), (31, 2, 2, 2)]
    + [(32, 2, u, s) for s in (3, 4) for u in range(3)]
)
EPS = 1e-6
VMEM_LIMIT = 67043328


def dot(a, b):
    return lax.dot_general(a, b, (((1,), (0,)), ((), ())), preferred_element_type=F32)


def dot_nt(a, b):
    return lax.dot_general(a, b, (((1,), (1,)), ((), ())), preferred_element_type=F32)


def dot_tn(a, b):
    return lax.dot_general(a, b, (((0,), (0,)), ((), ())), preferred_element_type=F32)


def sigmoid(g):
    return 0.5 * jnp.tanh(0.5 * g) + 0.5


def scale_of(wide):
    return lax.rsqrt(jnp.mean(wide * wide, -1, keepdims=True) + EPS)


def normed(wide):
    return (wide * scale_of(wide)).astype(BF)


def aligned(start, size):
    return pl.ds(pl.multiple_of(start, size), size)


def choose(j, table, do):
    keys = sorted(table)
    if len(keys) == 1:
        pl.when(j == keys[0])(lambda: do(table[keys[0]]))
    elif keys:
        mid = keys[len(keys) // 2]
        pl.when(j < mid)(lambda: choose(j, {k: v for k, v in table.items() if k < mid}, do))
        pl.when(j >= mid)(lambda: choose(j, {k: v for k, v in table.items() if k >= mid}, do))


def by_body(events, first, last):
    table = {}
    for at, *event in sorted(events, key=lambda e: (e[0], -e[3])):
        if first <= at < last:
            table.setdefault(at, []).append(event)
    return table


def kernel(
    n, x_hbm, dy_hbm, gate_hbm, up_hbm, down_hbm, dx_hbm, dgate_hbm, dup_hbm, ddown_hbm, h_hbm, gu_hbm,
    a1, y, g, w, acc, act0, act1, g0, g1, terms, slots, fin, io,
    sem, io_sem, gu_sem, out_sem, ag_recv, ag_send, side_recv, rs_recv, rs_send, credit,
):
    layers, chunks = w.shape[:2]
    tokens, d = y.shape
    fc = w.shape[-1]
    own = d // n
    half = fc // 2
    tm = tokens // TILES
    big = 2 * tm
    acts, gs = (act0, act1), (g0, g1)
    near = (n - 1) // 2

    me = lax.axis_index("dp")
    core = lax.axis_index("rep") % 2
    left, right = {"dp": (me + n - 1) % n}, {"dp": (me + 1) % n}
    partner = {"rep": lax.axis_index("rep") + 1 - 2 * core}
    owner = [(me + k) % n * own for k in range(n)]

    def remote(src, dst, send, recv, to):
        return pltpu.make_async_remote_copy(src, dst, send, recv, device_id=to, device_id_type=pl.DeviceIdType.MESH)

    ITEMS = [(0, c, m) for c in range(chunks) for m in range(2)] + [(0, slice(None), 2)] + [(l, c, slice(None)) for l in range(1, layers) for c in range(chunks)]

    def piece(i, rows):
        return w.at[(*ITEMS[i], rows, slice(None))]

    def gather(steps):
        for i, h in steps:
            far = near + i % 2
            for side, to in enumerate((right, left)):
                reach = (far, n - 1 - far)[side]
                if h > reach:
                    continue
                ref = piece(i, aligned(owner[(n - h) % n if side == 0 else h] + core * (own // 2), own // 2))
                at = side * far + h
                if h:
                    remote(ref, ref, ag_send.at[i], ag_recv.at[i, at - 1], to).wait_recv()
                if h < reach:
                    remote(ref, ref, ag_send.at[i], ag_recv.at[i, at], to).start()
                if h:
                    remote(ref, ref, ag_send.at[i], side_recv.at[i], partner).start()

    def arrived(*which):
        for i in which:
            ref = piece(i, pl.ds(0, (n - 1) * (own // 2)))
            pltpu.make_async_copy(ref, ref, side_recv.at[i]).wait()

    def reduce(turn, events):
        for p, u, s in events:
            far = near + (p + u) % 2
            for side, to in enumerate((right, left)):
                reach = (far, n - 1 - far)[side]
                if s >= reach:
                    continue
                at = side * far + s
                rows = aligned(owner[reach - s if side == 0 else n - reach + s], own)
                if s == 0:
                    if turn:
                        pl.semaphore_wait(credit.at[side, p, u], 1)
                    ref = terms.at[p, u, rows, :]
                else:
                    ref = slots.at[p, u, at - 1]
                    remote(ref, ref, rs_send.at[p, u], rs_recv.at[p, u, at - 1], to).wait_recv()
                    ref[...] = (ref[...].astype(F32) + terms[p, u, rows, :].astype(F32)).astype(BF)
                remote(ref, slots.at[p, u, at], rs_send.at[p, u], rs_recv.at[p, u, at], to).start()
            if s == near + 1:
                finish(turn, p, u, far)

    def down_out(l, p):
        return pltpu.make_async_copy(fin.at[p, 2], ddown_hbm.at[l, pl.ds(p * own, own), :], out_sem.at[p])

    def in_out(l, m, j):
        out = dgate_hbm if m == 0 else dup_hbm
        return pltpu.make_async_copy(fin.at[j, m], out.at[l, :, pl.ds(j * d, d)], out_sem.at[chunks + m * chunks + j])

    def finish(turn, p, u, far):
        l = layers - 1 - turn
        ends = [slots.at[p, u, far - 1], slots.at[p, u, n - 2]]
        for ref, at in zip(ends, (far - 1, n - 2)):
            remote(ref, ref, rs_send.at[p, u], rs_recv.at[p, u, at], right).wait_recv()
        if turn:
            (down_out(l + 1, p) if u == 2 else in_out(l + 1, u, p)).wait()
        rows = aligned(owner[0], own)
        fin[p, u] = (ends[0][...].astype(F32) + ends[1][...].astype(F32) + terms[p, u, rows, :].astype(F32)).astype(BF)
        ref = w.at[0, 0, 0, pl.ds(0, (n - 1) * own), :]
        pltpu.make_async_copy(ref, ref, rs_send.at[p, u]).wait()
        if l:
            pl.semaphore_signal(credit.at[0, p, u], 1, device_id=left, device_id_type=pl.DeviceIdType.MESH)
            pl.semaphore_signal(credit.at[1, p, u], 1, device_id=right, device_id_type=pl.DeviceIdType.MESH)
        if u == 2:
            down_out(l, p).start()
        if u < 2 and p == chunks - 1:
            low = lax.broadcasted_iota(jnp.int32, (own, 128), 1) < 64
            parts = [[fin[c, u, :, pl.ds(128 * e, 128)] for e in range(fc // 128)] for c in range(chunks)]
            for e in range(fc // 128):
                c0, c1, c2 = (parts[c][e].astype(F32) for c in range(chunks))
                c1 = pltpu.roll(c1, 64, 1)
                for k, (lo, hi) in enumerate(((c0, c1), (c2, c0), (c1, c2))):
                    j, at = divmod(3 * e + k, d // 128)
                    fin[j, u, :, pl.ds(128 * at, 128)] = jnp.where(low, lo, hi).astype(BF)
            for j in range(3):
                in_out(l, u, j).start()

    shards = (gate_hbm, up_hbm)
    raw = [
        pltpu.make_async_copy(shards[m].at[l, :, pl.ds(j * d, d)], terms.at[l, m, pl.ds(j * own, own), :], sem.at[2 + (l * 2 + m) * 3 + j])
        for l in range(layers) for m in range(2) for j in range(3)
    ]
    downs = [
        pltpu.make_async_copy(down_hbm.at[l, pl.ds(c * own, own), :], w.at[l, c, 2, aligned(owner[0], own), :], sem.at[2 + layers * 6 + l * 3 + c])
        for l in range(layers) for c in range(chunks)
    ]
    load_x, load_dy = pltpu.make_async_copy(x_hbm, a1, sem.at[0]), pltpu.make_async_copy(dy_hbm, y, sem.at[1])
    for copy in (*raw, *downs, load_x, load_dy):
        copy.start()
    barrier = pltpu.get_barrier_semaphore()
    for to in (left, right, partner):
        pl.semaphore_signal(barrier, 1, device_id=to, device_id_type=pl.DeviceIdType.MESH)
    for copy in (*raw, *downs):
        copy.wait()
    low = lax.broadcasted_iota(jnp.int32, (own, 128), 1) < 64
    for l in range(layers):
        for m in range(2):
            for e in range(fc // 128):
                parts = []
                for k in range(3):
                    j, at = divmod(3 * e + k, d // 128)
                    parts.append(terms[l, m, pl.ds(j * own, own), pl.ds(128 * at, 128)].astype(F32))
                k0, k1, k2 = parts
                mixed = (jnp.where(low, k0, k1), pltpu.roll(jnp.where(low, k2, k0), 64, 1), jnp.where(low, k1, k2))
                for c in range(chunks):
                    w[l, c, m, aligned(owner[0], own), pl.ds(128 * e, 128)] = mixed[c].astype(BF)
    pl.semaphore_wait(barrier, 3)

    gather(GATHER_START[0])
    load_x.wait()

    def norm_x(t, _):
        rows = aligned(t * tm, tm)
        a1[rows, :] = normed(a1[rows, :].astype(F32))
        return 0

    lax.fori_loop(0, TILES, norm_x, 0)
    for steps in GATHER_START[1:]:
        gather(steps)
    arrived(0, 1)

    def hidden_units(keep):
        def keep_out(b):
            return pltpu.make_async_copy(keep.at[b % 2], gu_hbm.at[pl.ds(2 * b, 2)], gu_sem.at[b % 2])

        def body(b, _):
            choose(b, GATHER_HIDDEN, gather)
            choose(b, {BODIES * c: (2 * c, 2 * c + 1) for c in range(1, chunks)}, lambda which: arrived(*which))
            pl.when(b >= 2)(lambda: keep_out(b - 2).wait())
            c = b // BODIES
            for k in range(2):
                rows = aligned(b % BODIES * big + k * tm, tm)
                at = a1[rows, :]
                for f in (0, half):
                    gate = dot(at, w[0, c, 0, :, f : f + half])
                    up = dot(at, w[0, c, 1, :, f : f + half])
                    keep[b % 2, k, 0, :, f : f + half] = gate
                    keep[b % 2, k, 1, :, f : f + half] = up
                    g[c, rows, f : f + half] = (gate * sigmoid(gate) * up).astype(BF)
            keep_out(b).start()
            return 0

        lax.fori_loop(0, chunks * BODIES, body, 0)
        for b in (chunks * BODIES - 2, chunks * BODIES - 1):
            keep_out(b).wait()

    def io_in(src, j):
        return pltpu.make_async_copy(src.at[aligned(j * big, big), :], io.at[j % 2], io_sem.at[0, j % 2])

    io_in(x_hbm, 0).start()
    io_in(x_hbm, 1).start()
    pl.run_scoped(hidden_units, pltpu.VMEM((2, 2, 2, tm, fc), F32))

    def backward(turn, a, gate_up, events):
        l = layers - 1 - turn
        tiles = chunks * TILES

        def grads_in(i, slot, f, kept):
            c, t = i // TILES, i % TILES
            rows = aligned(t * tm, tm)
            if kept is None:
                at = a[rows, :]
                gate = dot(at, w[l, c, 0, :, f : f + half])
                up = dot(at, w[l, c, 1, :, f : f + half])
            else:
                gate, up = kept[0, :, f : f + half], kept[1, :, f : f + half]
            dact = dot_nt(y[rows, :], w[l, c, 2, f : f + half, :]).astype(BF).astype(F32)
            s = sigmoid(gate)
            silu = gate * s
            acts[slot][:, f : f + half] = (silu * up).astype(BF)
            dgate = (dact * up * (s + silu * (1.0 - s))).astype(BF)
            dup = (dact * silu).astype(BF)
            gs[slot][:, f : f + half] = dgate
            gs[slot][:, fc + f : fc + f + half] = dup
            g[c, rows, f : f + half] = dgate
            g[c, rows, fc + f : fc + f + half] = dup

        def down_grad(i, slot):
            rows = aligned(i % TILES * tm, tm)
            acc[2] += dot_tn(acts[slot][...], y[rows, :])

        def in_grads(i, slot):
            rows = aligned(i % TILES * tm, tm)
            at = a[rows, :]
            acc[0] += dot_tn(at, gs[slot][:, :fc])
            acc[1] += dot_tn(at, gs[slot][:, fc:])

        def first_of(j):
            return jnp.minimum(2 * j + 1, tiles - 2)

        def block_in(j):
            return pltpu.make_async_copy(gu_hbm.at[pl.ds(first_of(j), 2)], gate_up.at[j % 3], gu_sem.at[j % 3])

        src = h_hbm if l else x_hbm
        io_in(src, 0).start()
        io_in(src, 1).start()
        if turn:
            first = pltpu.make_async_copy(gu_hbm.at[0], gate_up.at[2, 0], gu_sem.at[2])
            first.start()
            block_in(0).start()
            block_in(1).start()
            first.wait()
        for f in (0, half):
            grads_in(0, 0, f, gate_up.at[2, 0] if turn else None)

        def body(j, _):
            if not turn:
                choose(j, GATHER_BACK, gather)
                choose(j, {BODIES * c - 1: 3 * chunks - 2 + c for c in range(1, chunks)}, lambda i: arrived(i))
            choose(j, by_body(events, 0, chunks * BODIES), lambda e: run(turn, e))
            if turn:
                block_in(j).wait()
                pl.when(j + 2 < chunks * BODIES)(lambda: block_in(j + 2).start())
            for k in range(2):
                i = 2 * j + k
                ahead = jnp.minimum(i + 1, tiles - 1)
                kept = gate_up.at[j % 3, ahead - first_of(j) if k == 0 else 1] if turn else None
                grads_in(ahead, (k + 1) % 2, 0, kept)
                down_grad(i, k % 2)
                grads_in(ahead, (k + 1) % 2, half, kept)
                in_grads(i, k % 2)
            return 0

        def chunk(c, _):
            lax.fori_loop(c * BODIES, (c + 1) * BODIES, body, 0)
            for m in range(3):
                terms[c, m] = acc[m].astype(BF)
                acc[m] = jnp.zeros_like(acc[m])
            return 0

        lax.fori_loop(0, chunks, chunk, 0)

        def inputs(j, _):
            choose(j + chunks * BODIES, by_body(events, chunks * BODIES, LATE), lambda e: run(turn, e))
            io_in(src, j).wait()
            for k in range(2):
                rows = aligned(j * big + k * tm, tm)
                da = sum(dot_nt(g[c, rows, m * fc : (m + 1) * fc], w[l, c, m]) for c in range(chunks) for m in range(2))
                da = da.astype(BF).astype(F32)
                wide = io[j % 2, pl.ds(k * tm, tm), :].astype(F32)
                scale = scale_of(wide)
                along = jnp.mean(da * wide, -1, keepdims=True) * (scale * scale * scale)
                dh = (da * scale - wide * along).astype(BF).astype(F32)
                y[rows, :] = (y[rows, :].astype(F32) + dh).astype(BF)
            pl.when(j + 2 < BODIES)(lambda: io_in(src, j + 2).start())
            if l == 0:
                rows = aligned(j * big, big)
                pltpu.make_async_copy(y.at[rows, :], dx_hbm.at[rows, :], sem.at[0]).start()
            return 0

        lax.fori_loop(0, BODIES, inputs, 0)

    def run(turn, events):
        for *event, of in events:
            reduce(of, [event])

    for m in range(3):
        acc[m] = jnp.zeros_like(acc[m])

    def with_last(a2, out):
        def io_out(j):
            return pltpu.make_async_copy(out.at[j % 2], h_hbm.at[aligned(j * big, big), :], io_sem.at[1, j % 2])

        def down(j, _):
            choose(j, GATHER_DOWN, gather)
            pl.when(j == 0)(lambda: arrived(2 * chunks))
            io_in(x_hbm, j).wait()
            pl.when(j >= 2)(lambda: io_out(j - 2).wait())
            for k in range(2):
                rows = aligned(j * big + k * tm, tm)
                hidden = sum(dot(g[c, rows, :fc], w[0, c, 2]) for c in range(chunks))
                here = pl.ds(k * tm, tm)
                h = (io[j % 2, here, :].astype(F32) + hidden.astype(BF).astype(F32)).astype(BF)
                out[j % 2, here, :] = h
                a2[rows, :] = normed(h.astype(F32))
            io_out(j).start()
            pl.when(j + 2 < BODIES)(lambda: io_in(x_hbm, j + 2).start())
            return 0

        lax.fori_loop(0, BODIES, down, 0)
        io_out(BODIES - 2).wait()
        io_out(BODIES - 1).wait()
        load_dy.wait()
        arrived(2 * chunks + 1)
        backward(0, a2, None, [(*e, 0) for e in SUMS_FIRST if e[0] < LATE])

    pl.run_scoped(with_last, pltpu.VMEM((tokens, d), BF), pltpu.VMEM((2, big, d), BF))

    left_over = [(e[0] - LATE, *e[1:], 0) for e in SUMS_FIRST if e[0] >= LATE and e[3] < 3] + [(*e, 0) for e in SUMS_LEFT]
    second = left_over + [(*e, 1) for e in SUMS_SECOND]

    def with_first(gate_up):
        backward(1, a1, gate_up, second)

    pl.run_scoped(with_first, pltpu.VMEM((3, 2, 2, tm, fc), F32))

    for e in by_body(second, LATE, LATE + 1).values():
        run(1, sorted(e, key=lambda e: (e[2], e[0])))
    for p in range(chunks):
        down_out(0, p).wait()
    for m in range(2):
        for j in range(3):
            in_out(0, m, j).wait()
    pltpu.make_async_copy(y, dx_hbm, sem.at[0]).wait()
    for i in range(len(ITEMS)):
        ref = piece(i, pl.ds(0, (n - 1) * own))
        pltpu.make_async_copy(ref, ref, ag_send.at[i]).wait()


def layers_of(n, x, dy, gate, up, down):
    tokens, d = x.shape
    layers, own, ff = gate.shape
    fc = ff // CHUNKS
    tm = tokens // TILES
    items = 3 * CHUNKS + 1
    assert d == fc == n * own and down.shape == (layers, CHUNKS * own, d) and own == 64
    assert n == 8 and layers == 2
    hbm = pl.BlockSpec(memory_space=pl.ANY)
    dma = pltpu.SemaphoreType.DMA
    kept = jax.ShapeDtypeStruct((CHUNKS * TILES, 2, tm, fc), F32)
    return pl.pallas_call(
        functools.partial(kernel, n),
        out_shape=[*(jax.ShapeDtypeStruct(t.shape, BF) for t in (x, gate, up, down, x)), kept],
        in_specs=[hbm] * 5,
        out_specs=[hbm] * 6,
        scratch_shapes=[
            pltpu.VMEM((tokens, d), BF),
            pltpu.VMEM((tokens, d), BF),
            pltpu.VMEM((CHUNKS, tokens, 2 * fc), BF),
            pltpu.VMEM((layers, CHUNKS, 3, d, fc), BF),
            pltpu.VMEM((3, d, fc), F32),
            pltpu.VMEM((tm, fc), BF),
            pltpu.VMEM((tm, fc), BF),
            pltpu.VMEM((tm, 2 * fc), BF),
            pltpu.VMEM((tm, 2 * fc), BF),
            pltpu.VMEM((CHUNKS, 3, d, fc), BF),
            pltpu.VMEM((CHUNKS, 3, n - 1, own, fc), BF),
            pltpu.VMEM((CHUNKS, 3, own, fc), BF),
            pltpu.VMEM((2, 2 * tm, d), BF),
            dma((2 + layers * 9,)),
            dma((2, 2)),
            dma((3,)),
            dma((CHUNKS * 3,)),
            dma((items, n - 1)),
            dma((items,)),
            dma((items,)),
            dma((CHUNKS, 3, n - 1)),
            dma((CHUNKS, 3)),
            pltpu.SemaphoreType.REGULAR((2, CHUNKS, 3)),
        ],
        compiler_params=pltpu.CompilerParams(vmem_limit_bytes=VMEM_LIMIT, has_side_effects=True, collective_id=0),
        name="layers",
    )(x, dy, gate, up, down)[:4]


def copied(*arrays):
    parts = [t.reshape(-1, t.shape[-1]) for t in arrays]
    cuts = [8, *(1 for _ in parts[1:])]

    def kernel(*refs):
        k = len(parts)
        src, dst, bufs, sems = refs[:k], refs[k : 2 * k], refs[2 * k : 3 * k], refs[3 * k]
        moves = []
        for which, (s, t, buf, cut) in enumerate(zip(src, dst, bufs, cuts)):
            size = s.shape[0] // cut
            for j in range(cut):
                rows = pl.ds(j * size, size)
                at = sems.at[:, 8 * which + j]
                moves.append((pltpu.make_async_copy(s.at[rows], buf.at[rows], at.at[0]), pltpu.make_async_copy(buf.at[rows], t.at[rows], at.at[1])))
        for there, _ in moves:
            there.start()
        for there, back in moves:
            there.wait()
            back.start()
        for _, back in moves:
            back.wait()

    hbm = pl.BlockSpec(memory_space=pl.ANY)
    out = pl.pallas_call(
        kernel,
        out_shape=[jax.ShapeDtypeStruct(t.shape, t.dtype) for t in parts],
        in_specs=[hbm] * len(parts),
        out_specs=[hbm] * len(parts),
        scratch_shapes=[*(pltpu.VMEM(t.shape, t.dtype) for t in parts), pltpu.SemaphoreType.DMA((2, 8 * len(parts)))],
        name="outputs",
    )(*parts)
    return [t.reshape(like.shape) for t, like in zip(out, arrays)]


def solution(mesh):
    n = mesh.shape["dp"]
    assert mesh.shape["rep"] % 2 == 0

    def local(x, dy, gate, up, down):
        dx, *grads = copied(*layers_of(n, x[0], dy[0], gate, up, down))
        return dx[None], *grads

    both, rows = P(("rep", "dp"), None, None), P(None, "dp", None)
    grads = P("rep", "dp", None)
    return jax.shard_map(
        local, mesh=mesh, in_specs=(both, both, rows, rows, rows), out_specs=(both, grads, grads, grads), check_vma=False
    )
```

```python
import functools

import jax
import jax.numpy as jnp
from jax import lax
from jax.experimental import pallas as pl
from jax.experimental.pallas import tpu as pltpu
from jax.sharding import PartitionSpec as P

BF = jnp.bfloat16
F32 = jnp.float32
CHUNKS = 3
TILES = 16
BODIES = TILES // 2

GATHER_START = (
    ((0, 0), (1, 0), (2, 0), (3, 0), (4, 0), (5, 0)),
    ((0, 1), (1, 1), (3, 1), (4, 1), (5, 1)),
    ((0, 2), (1, 2), (2, 1), (6, 0)),
    ((0, 3), (1, 3), (2, 2), (3, 2), (5, 2), (6, 1)),
    ((0, 4), (1, 4), (2, 3), (3, 3)),
)
GATHER_HIDDEN = {
    0: ((4, 2),), 2: ((7, 0),), 4: ((6, 2),), 5: ((3, 4), (5, 3)), 6: ((2, 4),), 7: ((4, 3),), 8: ((7, 1),), 11: ((6, 3), (8, 0)),
    12: ((9, 0),), 13: ((5, 4),), 14: ((4, 4),), 16: ((7, 2),), 21: ((6, 4), (8, 1)), 22: ((9, 1),),
}
GATHER_DOWN = {1: ((7, 3),), 4: ((8, 2),), 6: ((7, 4),), 7: ((9, 2),)}
GATHER_BACK = {1: ((8, 3),), 3: ((9, 3),), 5: ((8, 4),), 11: ((9, 4),)}

SUMS_FIRST = [(BODIES * (p + 1) + 3 * s + u, p, u, s) for p in range(3) for s in range(5) for u in range(3)]
LATE = 4 * BODIES
SUMS_LEFT = [(1 + 4 * (s - 3) + u, 2, u, s) for s in (3, 4) for u in range(3)]
SUMS_SECOND = (
    [(8 + 4 * s + u, 0, u, s) for s in range(5) for u in range(3)]
    + [(17 + 4 * s + u, 1, u, s) for s in range(2) for u in range(3)]
    + [(25 + u, 1, u, 2) for u in range(3)] + [(28 + u, 1, u, 3) for u in range(3)] + [(31, 1, 0, 4), (31, 1, 1, 4), (32, 1, 2, 4)]
    + [(24, 2, 0, 0), (24, 2, 1, 0), (25, 2, 2, 0)] + [(27 + u, 2, u, 1) for u in range(3)] + [(30, 2, 0, 2), (31, 2, 1, 2), (31, 2, 2, 2)]
    + [(32, 2, u, s) for s in (3, 4) for u in range(3)]
)
EPS = 1e-6
VMEM_LIMIT = 67043328


def dot(a, b):
    return lax.dot_general(a, b, (((1,), (0,)), ((), ())), preferred_element_type=F32)


def dot_nt(a, b):
    return lax.dot_general(a, b, (((1,), (1,)), ((), ())), preferred_element_type=F32)


def dot_tn(a, b):
    return lax.dot_general(a, b, (((0,), (0,)), ((), ())), preferred_element_type=F32)


def sigmoid(g):
    return 0.5 * jnp.tanh(0.5 * g) + 0.5


def scale_of(wide):
    return lax.rsqrt(jnp.mean(wide * wide, -1, keepdims=True) + EPS)


def normed(wide):
    return (wide * scale_of(wide)).astype(BF)


def aligned(start, size):
    return pl.ds(pl.multiple_of(start, size), size)


def choose(j, table, do):
    keys = sorted(table)
    if len(keys) == 1:
        pl.when(j == keys[0])(lambda: do(table[keys[0]]))
    elif keys:
        mid = keys[len(keys) // 2]
        pl.when(j < mid)(lambda: choose(j, {k: v for k, v in table.items() if k < mid}, do))
        pl.when(j >= mid)(lambda: choose(j, {k: v for k, v in table.items() if k >= mid}, do))


def by_body(events, first, last):
    table = {}
    for at, *event in sorted(events, key=lambda e: (e[0], -e[3])):
        if first <= at < last:
            table.setdefault(at, []).append(event)
    return table


def kernel(
    n, x_hbm, dy_hbm, gate_hbm, up_hbm, down_hbm, dx_hbm, dgate_hbm, dup_hbm, ddown_hbm, h_hbm, gu_hbm,
    a1, y, g, w, acc, act0, act1, g0, g1, terms, slots, fin, io,
    sem, io_sem, gu_sem, out_sem, ag_recv, ag_send, side_recv, rs_recv, rs_send, credit,
):
    layers, chunks = w.shape[:2]
    tokens, d = y.shape
    fc = w.shape[-1]
    own = d // n
    half = fc // 2
    tm = tokens // TILES
    big = 2 * tm
    acts, gs = (act0, act1), (g0, g1)
    near = (n - 1) // 2

    me = lax.axis_index("dp")
    core = lax.axis_index("rep") % 2
    left, right = {"dp": (me + n - 1) % n}, {"dp": (me + 1) % n}
    partner = {"rep": lax.axis_index("rep") + 1 - 2 * core}
    owner = [(me + k) % n * own for k in range(n)]

    def remote(src, dst, send, recv, to):
        return pltpu.make_async_remote_copy(src, dst, send, recv, device_id=to, device_id_type=pl.DeviceIdType.MESH)

    ITEMS = [(0, c, m) for c in range(chunks) for m in range(2)] + [(0, slice(None), 2)] + [(l, c, slice(None)) for l in range(1, layers) for c in range(chunks)]

    def piece(i, rows):
        return w.at[(*ITEMS[i], rows, slice(None))]

    def gather(steps):
        for i, h in steps:
            far = near + i % 2
            for side, to in enumerate((right, left)):
                reach = (far, n - 1 - far)[side]
                if h > reach:
                    continue
                ref = piece(i, aligned(owner[(n - h) % n if side == 0 else h] + core * (own // 2), own // 2))
                at = side * far + h
                if h:
                    remote(ref, ref, ag_send.at[i], ag_recv.at[i, at - 1], to).wait_recv()
                if h < reach:
                    remote(ref, ref, ag_send.at[i], ag_recv.at[i, at], to).start()
                if h:
                    remote(ref, ref, ag_send.at[i], side_recv.at[i], partner).start()

    def arrived(*which):
        for i in which:
            ref = piece(i, pl.ds(0, (n - 1) * (own // 2)))
            pltpu.make_async_copy(ref, ref, side_recv.at[i]).wait()

    def reduce(turn, events):
        for p, u, s in events:
            far = near + (p + u) % 2
            for side, to in enumerate((right, left)):
                reach = (far, n - 1 - far)[side]
                if s >= reach:
                    continue
                at = side * far + s
                rows = aligned(owner[reach - s if side == 0 else n - reach + s], own)
                if s == 0:
                    if turn:
                        pl.semaphore_wait(credit.at[side, p, u], 1)
                    ref = terms.at[p, u, rows, :]
                else:
                    ref = slots.at[p, u, at - 1]
                    remote(ref, ref, rs_send.at[p, u], rs_recv.at[p, u, at - 1], to).wait_recv()
                    ref[...] = (ref[...].astype(F32) + terms[p, u, rows, :].astype(F32)).astype(BF)
                remote(ref, slots.at[p, u, at], rs_send.at[p, u], rs_recv.at[p, u, at], to).start()
            if s == near + 1:
                finish(turn, p, u, far)

    def down_out(l, p):
        return pltpu.make_async_copy(fin.at[p, 2], ddown_hbm.at[l, pl.ds(p * own, own), :], out_sem.at[p])

    def in_out(l, m, j):
        out = dgate_hbm if m == 0 else dup_hbm
        return pltpu.make_async_copy(fin.at[j, m], out.at[l, :, pl.ds(j * d, d)], out_sem.at[chunks + m * chunks + j])

    def finish(turn, p, u, far):
        l = layers - 1 - turn
        ends = [slots.at[p, u, far - 1], slots.at[p, u, n - 2]]
        for ref, at in zip(ends, (far - 1, n - 2)):
            remote(ref, ref, rs_send.at[p, u], rs_recv.at[p, u, at], right).wait_recv()
        if turn:
            (down_out(l + 1, p) if u == 2 else in_out(l + 1, u, p)).wait()
        rows = aligned(owner[0], own)
        fin[p, u] = (ends[0][...].astype(F32) + ends[1][...].astype(F32) + terms[p, u, rows, :].astype(F32)).astype(BF)
        ref = w.at[0, 0, 0, pl.ds(0, (n - 1) * own), :]
        pltpu.make_async_copy(ref, ref, rs_send.at[p, u]).wait()
        if l:
            pl.semaphore_signal(credit.at[0, p, u], 1, device_id=left, device_id_type=pl.DeviceIdType.MESH)
            pl.semaphore_signal(credit.at[1, p, u], 1, device_id=right, device_id_type=pl.DeviceIdType.MESH)
        if u == 2:
            down_out(l, p).start()
        if u < 2 and p == chunks - 1:
            low = lax.broadcasted_iota(jnp.int32, (own, 128), 1) < 64
            parts = [[fin[c, u, :, pl.ds(128 * e, 128)] for e in range(fc // 128)] for c in range(chunks)]
            for e in range(fc // 128):
                c0, c1, c2 = (parts[c][e].astype(F32) for c in range(chunks))
                c1 = pltpu.roll(c1, 64, 1)
                for k, (lo, hi) in enumerate(((c0, c1), (c2, c0), (c1, c2))):
                    j, at = divmod(3 * e + k, d // 128)
                    fin[j, u, :, pl.ds(128 * at, 128)] = jnp.where(low, lo, hi).astype(BF)
            for j in range(3):
                in_out(l, u, j).start()

    shards = (gate_hbm, up_hbm)
    raw = [
        pltpu.make_async_copy(shards[m].at[l, :, pl.ds(j * d, d)], terms.at[l, m, pl.ds(j * own, own), :], sem.at[2 + (l * 2 + m) * 3 + j])
        for l in range(layers) for m in range(2) for j in range(3)
    ]
    downs = [
        pltpu.make_async_copy(down_hbm.at[l, pl.ds(c * own, own), :], w.at[l, c, 2, aligned(owner[0], own), :], sem.at[2 + layers * 6 + l * 3 + c])
        for l in range(layers) for c in range(chunks)
    ]
    load_x, load_dy = pltpu.make_async_copy(x_hbm, a1, sem.at[0]), pltpu.make_async_copy(dy_hbm, y, sem.at[1])
    for copy in (*raw, *downs, load_x, load_dy):
        copy.start()
    barrier = pltpu.get_barrier_semaphore()
    for to in (left, right, partner):
        pl.semaphore_signal(barrier, 1, device_id=to, device_id_type=pl.DeviceIdType.MESH)
    for copy in (*raw, *downs):
        copy.wait()
    low = lax.broadcasted_iota(jnp.int32, (own, 128), 1) < 64
    for l in range(layers):
        for m in range(2):
            for e in range(fc // 128):
                parts = []
                for k in range(3):
                    j, at = divmod(3 * e + k, d // 128)
                    parts.append(terms[l, m, pl.ds(j * own, own), pl.ds(128 * at, 128)].astype(F32))
                k0, k1, k2 = parts
                mixed = (jnp.where(low, k0, k1), pltpu.roll(jnp.where(low, k2, k0), 64, 1), jnp.where(low, k1, k2))
                for c in range(chunks):
                    w[l, c, m, aligned(owner[0], own), pl.ds(128 * e, 128)] = mixed[c].astype(BF)
    pl.semaphore_wait(barrier, 3)

    gather(GATHER_START[0])
    load_x.wait()

    def norm_x(t, _):
        rows = aligned(t * tm, tm)
        a1[rows, :] = normed(a1[rows, :].astype(F32))
        return 0

    lax.fori_loop(0, TILES, norm_x, 0)
    for steps in GATHER_START[1:]:
        gather(steps)
    arrived(0, 1)

    def hidden_units(keep):
        def keep_out(b):
            return pltpu.make_async_copy(keep.at[b % 3], gu_hbm.at[pl.ds(2 * b, 2)], gu_sem.at[b % 3])

        def body(b, _):
            choose(b, GATHER_HIDDEN, gather)
            choose(b, {BODIES * c: (2 * c, 2 * c + 1) for c in range(1, chunks)}, lambda which: arrived(*which))
            pl.when(b >= 3)(lambda: keep_out(b - 3).wait())
            c = b // BODIES
            for k in range(2):
                rows = aligned(b % BODIES * big + k * tm, tm)
                at = a1[rows, :]
                for f in (0, half):
                    gate = dot(at, w[0, c, 0, :, f : f + half])
                    up = dot(at, w[0, c, 1, :, f : f + half])
                    keep[b % 3, k, 0, :, f : f + half] = gate
                    keep[b % 3, k, 1, :, f : f + half] = up
                    g[c, rows, f : f + half] = (gate * sigmoid(gate) * up).astype(BF)
            keep_out(b).start()
            return 0

        lax.fori_loop(0, chunks * BODIES, body, 0)
        for b in range(chunks * BODIES - 3, chunks * BODIES):
            keep_out(b).wait()

    def io_in(src, j):
        return pltpu.make_async_copy(src.at[aligned(j * big, big), :], io.at[j % 2], io_sem.at[0, j % 2])

    io_in(x_hbm, 0).start()
    io_in(x_hbm, 1).start()
    pl.run_scoped(hidden_units, pltpu.VMEM((3, 2, 2, tm, fc), F32))

    def backward(turn, a, gate_up, events, pending):
        l = layers - 1 - turn
        tiles = chunks * TILES

        def grads_in(i, slot, f, kept):
            c, t = i // TILES, i % TILES
            rows = aligned(t * tm, tm)
            if kept is None:
                at = a[rows, :]
                gate = dot(at, w[l, c, 0, :, f : f + half])
                up = dot(at, w[l, c, 1, :, f : f + half])
            else:
                gate, up = kept[0, :, f : f + half], kept[1, :, f : f + half]
            dact = dot_nt(y[rows, :], w[l, c, 2, f : f + half, :]).astype(BF).astype(F32)
            s = sigmoid(gate)
            silu = gate * s
            acts[slot][:, f : f + half] = (silu * up).astype(BF)
            dgate = (dact * up * (s + silu * (1.0 - s))).astype(BF)
            dup = (dact * silu).astype(BF)
            gs[slot][:, f : f + half] = dgate
            gs[slot][:, fc + f : fc + f + half] = dup
            g[c, rows, f : f + half] = dgate
            g[c, rows, fc + f : fc + f + half] = dup

        def down_grad(i, slot):
            rows = aligned(i % TILES * tm, tm)
            acc[2] += dot_tn(acts[slot][...], y[rows, :])

        def in_grads(i, slot):
            rows = aligned(i % TILES * tm, tm)
            at = a[rows, :]
            acc[0] += dot_tn(at, gs[slot][:, :fc])
            acc[1] += dot_tn(at, gs[slot][:, fc:])

        def first_of(j):
            return jnp.minimum(2 * j + 1, tiles - 2)

        def block_in(j):
            return pltpu.make_async_copy(gu_hbm.at[pl.ds(first_of(j), 2)], gate_up.at[j % 3], gu_sem.at[j % 3])

        src = h_hbm if l else x_hbm
        io_in(src, 0).start()
        io_in(src, 1).start()
        if turn:
            for copy in first_tile:
                copy.wait()
            block_in(0).start()
            block_in(1).start()
        for f in (0, half):
            grads_in(0, 0, f, acc.at[0, pl.ds(0, 2 * tm), :].reshape(2, tm, fc) if turn else None)
        if turn:
            acc[0] = jnp.zeros_like(acc[0])

        def body(j, _):
            if not turn:
                choose(j, GATHER_BACK, gather)
                choose(j, {BODIES * c - 1: 3 * chunks - 2 + c for c in range(1, chunks)}, lambda i: arrived(i))
            choose(j, by_body(events, 0, chunks * BODIES), lambda e: run(turn, e))
            if turn:
                block_in(j).wait()
                pl.when(j + 2 < chunks * BODIES)(lambda: block_in(j + 2).start())
            for k in range(2):
                i = 2 * j + k
                ahead = jnp.minimum(i + 1, tiles - 1)
                kept = gate_up.at[j % 3, ahead - first_of(j) if k == 0 else 1] if turn else None
                grads_in(ahead, (k + 1) % 2, 0, kept)
                down_grad(i, k % 2)
                grads_in(ahead, (k + 1) % 2, half, kept)
                in_grads(i, k % 2)
            return 0

        def chunk(c, _):
            lax.fori_loop(c * BODIES, (c + 1) * BODIES, body, 0)
            for m in range(3):
                terms[c, m] = acc[m].astype(BF)
                acc[m] = jnp.zeros_like(acc[m])
            return 0

        lax.fori_loop(0, chunks, chunk, 0)
        for copy in pending:
            copy.wait()
        for copy in first_tile if not turn else ():
            copy.start()

        def inputs(j, _):
            choose(j + chunks * BODIES, by_body(events, chunks * BODIES, LATE), lambda e: run(turn, e))
            io_in(src, j).wait()
            for k in range(2):
                rows = aligned(j * big + k * tm, tm)
                da = sum(dot_nt(g[c, rows, m * fc : (m + 1) * fc], w[l, c, m]) for c in range(chunks) for m in range(2))
                da = da.astype(BF).astype(F32)
                wide = io[j % 2, pl.ds(k * tm, tm), :].astype(F32)
                scale = scale_of(wide)
                along = jnp.mean(da * wide, -1, keepdims=True) * (scale * scale * scale)
                dh = (da * scale - wide * along).astype(BF).astype(F32)
                y[rows, :] = (y[rows, :].astype(F32) + dh).astype(BF)
            pl.when(j + 2 < BODIES)(lambda: io_in(src, j + 2).start())
            if l == 0:
                rows = aligned(j * big, big)
                pltpu.make_async_copy(y.at[rows, :], dx_hbm.at[rows, :], sem.at[0]).start()
            return 0

        lax.fori_loop(0, BODIES, inputs, 0)

    def run(turn, events):
        for *event, of in events:
            reduce(of, [event])

    for m in range(3):
        acc[m] = jnp.zeros_like(acc[m])
    first_tile = [pltpu.make_async_copy(gu_hbm.at[0, m], acc.at[0, pl.ds(m * tm, tm), :], gu_sem.at[m]) for m in range(2)]

    def with_last(a2, out):
        def io_out(j):
            return pltpu.make_async_copy(out.at[j % 2], h_hbm.at[aligned(j * big, big), :], io_sem.at[1, j % 2])

        def down(j, _):
            choose(j, GATHER_DOWN, gather)
            pl.when(j == 0)(lambda: arrived(2 * chunks))
            io_in(x_hbm, j).wait()
            pl.when(j >= 2)(lambda: io_out(j - 2).wait())
            for k in range(2):
                rows = aligned(j * big + k * tm, tm)
                hidden = sum(dot(g[c, rows, :fc], w[0, c, 2]) for c in range(chunks))
                here = pl.ds(k * tm, tm)
                h = (io[j % 2, here, :].astype(F32) + hidden.astype(BF).astype(F32)).astype(BF)
                out[j % 2, here, :] = h
                a2[rows, :] = normed(h.astype(F32))
            io_out(j).start()
            pl.when(j + 2 < BODIES)(lambda: io_in(x_hbm, j + 2).start())
            return 0

        lax.fori_loop(0, BODIES, down, 0)
        load_dy.wait()
        arrived(2 * chunks + 1)
        backward(0, a2, None, [(*e, 0) for e in SUMS_FIRST if e[0] < LATE], [io_out(BODIES - 2), io_out(BODIES - 1)])

    pl.run_scoped(with_last, pltpu.VMEM((tokens, d), BF), pltpu.VMEM((2, big, d), BF))

    left_over = [(e[0] - LATE, *e[1:], 0) for e in SUMS_FIRST if e[0] >= LATE and e[3] < 3] + [(*e, 0) for e in SUMS_LEFT]
    second = left_over + [(*e, 1) for e in SUMS_SECOND]

    def with_first(gate_up):
        backward(1, a1, gate_up, second, ())

    pl.run_scoped(with_first, pltpu.VMEM((3, 2, 2, tm, fc), F32))

    for e in by_body(second, LATE, LATE + 1).values():
        run(1, sorted(e, key=lambda e: (e[2], e[0])))
    for p in range(chunks):
        down_out(0, p).wait()
    for m in range(2):
        for j in range(3):
            in_out(0, m, j).wait()
    pltpu.make_async_copy(y, dx_hbm, sem.at[0]).wait()
    for i in range(len(ITEMS)):
        ref = piece(i, pl.ds(0, (n - 1) * own))
        pltpu.make_async_copy(ref, ref, ag_send.at[i]).wait()


def layers_of(n, x, dy, gate, up, down):
    tokens, d = x.shape
    layers, own, ff = gate.shape
    fc = ff // CHUNKS
    tm = tokens // TILES
    items = 3 * CHUNKS + 1
    assert d == fc == n * own and down.shape == (layers, CHUNKS * own, d) and own == 64
    assert n == 8 and layers == 2
    hbm = pl.BlockSpec(memory_space=pl.ANY)
    dma = pltpu.SemaphoreType.DMA
    kept = jax.ShapeDtypeStruct((CHUNKS * TILES, 2, tm, fc), F32)
    return pl.pallas_call(
        functools.partial(kernel, n),
        out_shape=[*(jax.ShapeDtypeStruct(t.shape, BF) for t in (x, gate, up, down, x)), kept],
        in_specs=[hbm] * 5,
        out_specs=[hbm] * 6,
        scratch_shapes=[
            pltpu.VMEM((tokens, d), BF),
            pltpu.VMEM((tokens, d), BF),
            pltpu.VMEM((CHUNKS, tokens, 2 * fc), BF),
            pltpu.VMEM((layers, CHUNKS, 3, d, fc), BF),
            pltpu.VMEM((3, d, fc), F32),
            pltpu.VMEM((tm, fc), BF),
            pltpu.VMEM((tm, fc), BF),
            pltpu.VMEM((tm, 2 * fc), BF),
            pltpu.VMEM((tm, 2 * fc), BF),
            pltpu.VMEM((CHUNKS, 3, d, fc), BF),
            pltpu.VMEM((CHUNKS, 3, n - 1, own, fc), BF),
            pltpu.VMEM((CHUNKS, 3, own, fc), BF),
            pltpu.VMEM((2, 2 * tm, d), BF),
            dma((2 + layers * 9,)),
            dma((2, 2)),
            dma((3,)),
            dma((CHUNKS * 3,)),
            dma((items, n - 1)),
            dma((items,)),
            dma((items,)),
            dma((CHUNKS, 3, n - 1)),
            dma((CHUNKS, 3)),
            pltpu.SemaphoreType.REGULAR((2, CHUNKS, 3)),
        ],
        compiler_params=pltpu.CompilerParams(vmem_limit_bytes=VMEM_LIMIT, has_side_effects=True, collective_id=0),
        name="layers",
    )(x, dy, gate, up, down)[:4]


def copied(*arrays):
    parts = [t.reshape(-1, t.shape[-1]) for t in arrays]
    cuts = [8, *(1 for _ in parts[1:])]

    def kernel(*refs):
        k = len(parts)
        src, dst, bufs, sems = refs[:k], refs[k : 2 * k], refs[2 * k : 3 * k], refs[3 * k]
        moves = []
        for which, (s, t, buf, cut) in enumerate(zip(src, dst, bufs, cuts)):
            size = s.shape[0] // cut
            for j in range(cut):
                rows = pl.ds(j * size, size)
                at = sems.at[:, 8 * which + j]
                moves.append((pltpu.make_async_copy(s.at[rows], buf.at[rows], at.at[0]), pltpu.make_async_copy(buf.at[rows], t.at[rows], at.at[1])))
        for there, _ in moves:
            there.start()
        for there, back in moves:
            there.wait()
            back.start()
        for _, back in moves:
            back.wait()

    hbm = pl.BlockSpec(memory_space=pl.ANY)
    out = pl.pallas_call(
        kernel,
        out_shape=[jax.ShapeDtypeStruct(t.shape, t.dtype) for t in parts],
        in_specs=[hbm] * len(parts),
        out_specs=[hbm] * len(parts),
        scratch_shapes=[*(pltpu.VMEM(t.shape, t.dtype) for t in parts), pltpu.SemaphoreType.DMA((2, 8 * len(parts)))],
        name="outputs",
    )(*parts)
    return [t.reshape(like.shape) for t, like in zip(out, arrays)]


def solution(mesh):
    n = mesh.shape["dp"]
    assert mesh.shape["rep"] % 2 == 0

    def local(x, dy, gate, up, down):
        dx, *grads = copied(*layers_of(n, x[0], dy[0], gate, up, down))
        return dx[None], *grads

    both, rows = P(("rep", "dp"), None, None), P(None, "dp", None)
    grads = P("rep", "dp", None)
    return jax.shard_map(
        local, mesh=mesh, in_specs=(both, both, rows, rows, rows), out_specs=(both, grads, grads, grads), check_vma=False
    )
```

```python
import functools

import jax
import jax.numpy as jnp
from jax import lax
from jax.experimental import pallas as pl
from jax.experimental.pallas import tpu as pltpu
from jax.sharding import PartitionSpec as P

BF = jnp.bfloat16
F32 = jnp.float32
CHUNKS = 3
TILES = 16
BODIES = TILES // 2

GATHER_START = (
    ((0, 0), (1, 0), (2, 0), (3, 0), (4, 0), (5, 0)),
    ((0, 1), (1, 1), (3, 1), (4, 1), (5, 1)),
    ((0, 2), (1, 2), (2, 1), (6, 0)),
    ((0, 3), (1, 3), (2, 2), (3, 2), (5, 2), (6, 1)),
    ((0, 4), (1, 4), (2, 3), (3, 3)),
)
GATHER_HIDDEN = {
    0: ((4, 2),), 2: ((7, 0),), 4: ((6, 2),), 5: ((3, 4), (5, 3)), 6: ((2, 4),), 7: ((4, 3),), 8: ((7, 1),), 11: ((6, 3), (8, 0)),
    12: ((9, 0),), 13: ((5, 4),), 14: ((4, 4),), 16: ((7, 2),), 21: ((6, 4), (8, 1)), 22: ((9, 1),),
}
GATHER_DOWN = {1: ((7, 3),), 4: ((8, 2),), 6: ((7, 4),), 7: ((9, 2),)}
GATHER_BACK = {0: ((8, 3),), 2: ((8, 4), (9, 3)), 4: ((9, 4),)}
WIDTHS = (4, 2)

SUMS = {
    4: ((0, 0, 0, 0),), 6: ((0, 0, 1, 0), (0, 0, 2, 0),), 7: ((0, 0, 0, 1),), 8: ((0, 1, 0, 0), (0, 1, 2, 0),),
    10: ((0, 0, 1, 1), (0, 0, 2, 1), (0, 1, 0, 1), (0, 1, 2, 1),), 11: ((0, 1, 1, 0),), 12: ((0, 0, 1, 2), (0, 0, 2, 2),), 13: ((0, 2, 1, 0),),
    14: ((0, 1, 1, 1), (0, 2, 0, 0), (0, 2, 2, 0),), 15: ((0, 0, 2, 3), (0, 0, 0, 2), (0, 1, 2, 2),), 16: ((0, 1, 0, 2), (0, 2, 1, 1),),
    18: ((0, 0, 2, 4), (0, 2, 0, 1),), 19: ((0, 2, 2, 1),), 20: ((0, 0, 0, 3),), 21: ((0, 1, 1, 2),), 22: ((0, 1, 0, 3), (0, 2, 0, 2),),
    23: ((0, 0, 0, 4), (0, 0, 1, 3), (0, 2, 1, 2), (0, 2, 2, 2),), 25: ((0, 1, 0, 4), (0, 1, 1, 3),), 26: ((0, 1, 2, 3),),
    27: ((0, 0, 1, 4), (0, 2, 0, 3),), 28: ((0, 1, 1, 4), (1, 0, 2, 0),), 29: ((1, 0, 0, 0),), 30: ((0, 1, 2, 4), (0, 2, 0, 4), (1, 0, 1, 0),),
    31: ((1, 0, 2, 1),), 32: ((1, 0, 0, 1),), 33: ((1, 0, 1, 1),), 34: ((0, 2, 2, 3), (1, 0, 2, 2),), 35: ((1, 0, 0, 2),),
    36: ((1, 0, 1, 2), (1, 1, 0, 0),), 37: ((0, 2, 2, 4),), 38: ((0, 2, 1, 3), (1, 1, 1, 0), (1, 1, 2, 0),), 39: ((1, 0, 0, 3), (1, 0, 2, 3),),
    40: ((1, 0, 1, 3),), 41: ((0, 2, 1, 4), (1, 1, 0, 1),), 42: ((1, 1, 1, 1),), 43: ((1, 0, 0, 4), (1, 1, 2, 1),),
    44: ((1, 0, 1, 4), (1, 0, 2, 4), (1, 2, 0, 0), (1, 2, 1, 0),), 45: ((1, 1, 0, 2), (1, 2, 2, 0),), 46: ((1, 1, 2, 2),),
    47: ((1, 2, 0, 1), (1, 2, 1, 1),), 48: ((1, 2, 2, 1),), 49: ((1, 1, 1, 2), (1, 2, 0, 2),), 50: ((1, 2, 1, 2), (1, 2, 2, 2),),
    51: ((1, 1, 0, 3), (1, 1, 1, 3), (1, 1, 2, 3), (1, 2, 0, 3),),
    52: ((1, 2, 1, 3), (1, 2, 2, 3), (1, 1, 0, 4), (1, 1, 1, 4), (1, 1, 2, 4), (1, 2, 0, 4), (1, 2, 1, 4), (1, 2, 2, 4),),
}
EPS = 1e-6
VMEM_LIMIT = 67043328


def dot(a, b):
    return lax.dot_general(a, b, (((1,), (0,)), ((), ())), preferred_element_type=F32)


def dot_nt(a, b):
    return lax.dot_general(a, b, (((1,), (1,)), ((), ())), preferred_element_type=F32)


def dot_tn(a, b):
    return lax.dot_general(a, b, (((0,), (0,)), ((), ())), preferred_element_type=F32)


def sigmoid(g):
    return 0.5 * jnp.tanh(0.5 * g) + 0.5


def scale_of(wide):
    return lax.rsqrt(jnp.mean(wide * wide, -1, keepdims=True) + EPS)


def normed(wide):
    return (wide * scale_of(wide)).astype(BF)


def aligned(start, size):
    return pl.ds(pl.multiple_of(start, size), size)


def choose(j, table, do):
    keys = sorted(table)
    if len(keys) == 1:
        pl.when(j == keys[0])(lambda: do(table[keys[0]]))
    elif keys:
        mid = keys[len(keys) // 2]
        pl.when(j < mid)(lambda: choose(j, {k: v for k, v in table.items() if k < mid}, do))
        pl.when(j >= mid)(lambda: choose(j, {k: v for k, v in table.items() if k >= mid}, do))


def kernel(
    n, x_hbm, dy_hbm, gate_hbm, up_hbm, down_hbm, dx_hbm, dgate_hbm, dup_hbm, ddown_hbm, h_hbm, gu_hbm,
    a1, y, g, w, acc, act0, act1, g0, g1, terms, slots, fin, io,
    sem, io_sem, gu_sem, out_sem, ag_recv, ag_send, side_recv, rs_recv, rs_send, credit,
):
    layers, chunks = w.shape[:2]
    tokens, d = y.shape
    fc = w.shape[-1]
    own = d // n
    half = fc // 2
    tm = tokens // TILES
    big = 2 * tm
    acts, gs = (act0, act1), (g0, g1)
    near = (n - 1) // 2

    me = lax.axis_index("dp")
    core = lax.axis_index("rep") % 2
    left, right = {"dp": (me + n - 1) % n}, {"dp": (me + 1) % n}
    partner = {"rep": lax.axis_index("rep") + 1 - 2 * core}
    owner = [(me + k) % n * own for k in range(n)]

    def remote(src, dst, send, recv, to):
        return pltpu.make_async_remote_copy(src, dst, send, recv, device_id=to, device_id_type=pl.DeviceIdType.MESH)

    ITEMS = [(0, c, m) for c in range(chunks) for m in range(2)] + [(0, slice(None), 2)] + [(l, c, slice(None)) for l in range(1, layers) for c in range(chunks)]

    def piece(i, rows):
        return w.at[(*ITEMS[i], rows, slice(None))]

    def gather(steps):
        for i, h in steps:
            far = near + i % 2
            for side, to in enumerate((right, left)):
                reach = (far, n - 1 - far)[side]
                if h > reach:
                    continue
                ref = piece(i, aligned(owner[(n - h) % n if side == 0 else h] + core * (own // 2), own // 2))
                at = side * far + h
                if h:
                    remote(ref, ref, ag_send.at[i], ag_recv.at[i, at - 1], to).wait_recv()
                if h < reach:
                    remote(ref, ref, ag_send.at[i], ag_recv.at[i, at], to).start()
                if h:
                    remote(ref, ref, ag_send.at[i], side_recv.at[i], partner).start()

    def arrived(*which):
        for i in which:
            ref = piece(i, pl.ds(0, (n - 1) * (own // 2)))
            pltpu.make_async_copy(ref, ref, side_recv.at[i]).wait()

    def reduce(events):
        for turn, p, u, s in events:
            far = near + (p + u) % 2
            for side, to in enumerate((right, left)):
                reach = (far, n - 1 - far)[side]
                if s >= reach:
                    continue
                at = side * far + s
                rows = aligned(owner[reach - s if side == 0 else n - reach + s], own)
                if s == 0:
                    if turn:
                        pl.semaphore_wait(credit.at[side, p, u], 1)
                    ref = terms.at[p, u, rows, :]
                else:
                    ref = slots.at[p, u, at - 1]
                    remote(ref, ref, rs_send.at[p, u], rs_recv.at[p, u, at - 1], to).wait_recv()
                    ref[...] = (ref[...].astype(F32) + terms[p, u, rows, :].astype(F32)).astype(BF)
                remote(ref, slots.at[p, u, at], rs_send.at[p, u], rs_recv.at[p, u, at], to).start()
            if s == near + 1:
                finish(turn, p, u, far)

    def down_out(l, p):
        return pltpu.make_async_copy(fin.at[p, 2], ddown_hbm.at[l, pl.ds(p * own, own), :], out_sem.at[p])

    def in_out(l, m, j):
        out = dgate_hbm if m == 0 else dup_hbm
        return pltpu.make_async_copy(fin.at[j, m], out.at[l, :, pl.ds(j * d, d)], out_sem.at[chunks + m * chunks + j])

    def finish(turn, p, u, far):
        l = layers - 1 - turn
        ends = [slots.at[p, u, far - 1], slots.at[p, u, n - 2]]
        for ref, at in zip(ends, (far - 1, n - 2)):
            remote(ref, ref, rs_send.at[p, u], rs_recv.at[p, u, at], right).wait_recv()
        if turn:
            (down_out(l + 1, p) if u == 2 else in_out(l + 1, u, p)).wait()
        rows = aligned(owner[0], own)
        fin[p, u] = (ends[0][...].astype(F32) + ends[1][...].astype(F32) + terms[p, u, rows, :].astype(F32)).astype(BF)
        ref = w.at[0, 0, 0, pl.ds(0, (n - 1) * own), :]
        pltpu.make_async_copy(ref, ref, rs_send.at[p, u]).wait()
        if l:
            pl.semaphore_signal(credit.at[0, p, u], 1, device_id=left, device_id_type=pl.DeviceIdType.MESH)
            pl.semaphore_signal(credit.at[1, p, u], 1, device_id=right, device_id_type=pl.DeviceIdType.MESH)
        if u == 2:
            down_out(l, p).start()
        if u < 2 and p == chunks - 1:
            low = lax.broadcasted_iota(jnp.int32, (own, 128), 1) < 64
            parts = [[fin[c, u, :, pl.ds(128 * e, 128)] for e in range(fc // 128)] for c in range(chunks)]
            for e in range(fc // 128):
                c0, c1, c2 = (parts[c][e].astype(F32) for c in range(chunks))
                c1 = pltpu.roll(c1, 64, 1)
                for k, (lo, hi) in enumerate(((c0, c1), (c2, c0), (c1, c2))):
                    j, at = divmod(3 * e + k, d // 128)
                    fin[j, u, :, pl.ds(128 * at, 128)] = jnp.where(low, lo, hi).astype(BF)
            for j in range(3):
                in_out(l, u, j).start()

    shards = (gate_hbm, up_hbm)
    raw = [
        pltpu.make_async_copy(shards[m].at[l, :, pl.ds(j * d, d)], terms.at[l, m, pl.ds(j * own, own), :], sem.at[2 + (l * 2 + m) * 3 + j])
        for l in range(layers) for m in range(2) for j in range(3)
    ]
    downs = [
        pltpu.make_async_copy(down_hbm.at[l, pl.ds(c * own, own), :], w.at[l, c, 2, aligned(owner[0], own), :], sem.at[2 + layers * 6 + l * 3 + c])
        for l in range(layers) for c in range(chunks)
    ]
    load_x, load_dy = pltpu.make_async_copy(x_hbm, a1, sem.at[0]), pltpu.make_async_copy(dy_hbm, y, sem.at[1])
    for copy in (*raw, *downs, load_x, load_dy):
        copy.start()
    barrier = pltpu.get_barrier_semaphore()
    for to in (left, right, partner):
        pl.semaphore_signal(barrier, 1, device_id=to, device_id_type=pl.DeviceIdType.MESH)
    for copy in (*raw, *downs):
        copy.wait()
    low = lax.broadcasted_iota(jnp.int32, (own, 128), 1) < 64
    for l in range(layers):
        for m in range(2):
            for e in range(fc // 128):
                parts = []
                for k in range(3):
                    j, at = divmod(3 * e + k, d // 128)
                    parts.append(terms[l, m, pl.ds(j * own, own), pl.ds(128 * at, 128)].astype(F32))
                k0, k1, k2 = parts
                mixed = (jnp.where(low, k0, k1), pltpu.roll(jnp.where(low, k2, k0), 64, 1), jnp.where(low, k1, k2))
                for c in range(chunks):
                    w[l, c, m, aligned(owner[0], own), pl.ds(128 * e, 128)] = mixed[c].astype(BF)
    pl.semaphore_wait(barrier, 3)

    gather(GATHER_START[0])
    load_x.wait()

    def norm_x(t, _):
        rows = aligned(t * tm, tm)
        a1[rows, :] = normed(a1[rows, :].astype(F32))
        return 0

    lax.fori_loop(0, TILES, norm_x, 0)
    for steps in GATHER_START[1:]:
        gather(steps)
    arrived(0, 1)

    def hidden_units(keep):
        def keep_out(b):
            return pltpu.make_async_copy(keep.at[b % 3], gu_hbm.at[pl.ds(2 * b, 2)], gu_sem.at[b % 3])

        def body(b, _):
            choose(b, GATHER_HIDDEN, gather)
            choose(b, {BODIES * c: (2 * c, 2 * c + 1) for c in range(1, chunks)}, lambda which: arrived(*which))
            pl.when(b >= 3)(lambda: keep_out(b - 3).wait())
            c = b // BODIES
            for k in range(2):
                rows = aligned(b % BODIES * big + k * tm, tm)
                at = a1[rows, :]
                for f in (0, half):
                    gate = dot(at, w[0, c, 0, :, f : f + half])
                    up = dot(at, w[0, c, 1, :, f : f + half])
                    keep[b % 3, k, 0, :, f : f + half] = gate
                    keep[b % 3, k, 1, :, f : f + half] = up
                    g[c, rows, f : f + half] = (gate * sigmoid(gate) * up).astype(BF)
            keep_out(b).start()
            return 0

        lax.fori_loop(0, chunks * BODIES, body, 0)
        for b in range(chunks * BODIES - 3, chunks * BODIES):
            keep_out(b).wait()

    def io_in(src, j):
        return pltpu.make_async_copy(src.at[aligned(j * big, big), :], io.at[j % 2], io_sem.at[0, j % 2])

    io_in(x_hbm, 0).start()
    io_in(x_hbm, 1).start()
    pl.run_scoped(hidden_units, pltpu.VMEM((3, 2, 2, tm, fc), F32))

    def backward(turn, a, gate_up, start, pending):
        l = layers - 1 - turn
        width = WIDTHS[turn]
        bodies = TILES // width
        table = {at - start: steps for at, steps in SUMS.items() if at >= start}
        loop = chunks * bodies
        tiles = chunks * TILES

        def grads_in(i, slot, f, kept):
            c, t = i // TILES, i % TILES
            rows = aligned(t * tm, tm)
            if kept is None:
                at = a[rows, :]
                gate = dot(at, w[l, c, 0, :, f : f + half])
                up = dot(at, w[l, c, 1, :, f : f + half])
            else:
                gate, up = kept[0, :, f : f + half], kept[1, :, f : f + half]
            dact = dot_nt(y[rows, :], w[l, c, 2, f : f + half, :]).astype(BF).astype(F32)
            s = sigmoid(gate)
            silu = gate * s
            acts[slot][:, f : f + half] = (silu * up).astype(BF)
            dgate = (dact * up * (s + silu * (1.0 - s))).astype(BF)
            dup = (dact * silu).astype(BF)
            gs[slot][:, f : f + half] = dgate
            gs[slot][:, fc + f : fc + f + half] = dup
            g[c, rows, f : f + half] = dgate
            g[c, rows, fc + f : fc + f + half] = dup

        def down_grad(i, slot):
            rows = aligned(i % TILES * tm, tm)
            acc[2] += dot_tn(acts[slot][...], y[rows, :])

        def in_grads(i, slot):
            rows = aligned(i % TILES * tm, tm)
            at = a[rows, :]
            acc[0] += dot_tn(at, gs[slot][:, :fc])
            acc[1] += dot_tn(at, gs[slot][:, fc:])

        def first_of(j):
            return jnp.minimum(2 * j + 1, tiles - 2)

        def block_in(j):
            return pltpu.make_async_copy(gu_hbm.at[pl.ds(first_of(j), 2)], gate_up.at[j % 3], gu_sem.at[j % 3])

        src = h_hbm if l else x_hbm
        io_in(src, 0).start()
        io_in(src, 1).start()
        if turn:
            for copy in first_tile:
                copy.wait()
            block_in(0).start()
            block_in(1).start()
        for f in (0, half):
            grads_in(0, 0, f, acc.at[0, pl.ds(0, 2 * tm), :].reshape(2, tm, fc) if turn else None)
        if turn:
            acc[0] = jnp.zeros_like(acc[0])

        def body(j, _):
            if not turn:
                choose(j, GATHER_BACK, gather)
                choose(j, {bodies * c - 1: 3 * chunks - 2 + c for c in range(1, chunks)}, lambda i: arrived(i))
            choose(j, {at: steps for at, steps in table.items() if at < loop}, reduce)
            if turn:
                block_in(j).wait()
                pl.when(j + 2 < loop)(lambda: block_in(j + 2).start())
            for k in range(width):
                i = width * j + k
                ahead = jnp.minimum(i + 1, tiles - 1)
                kept = gate_up.at[j % 3, ahead - first_of(j) if k == 0 else 1] if turn else None
                grads_in(ahead, (k + 1) % 2, 0, kept)
                down_grad(i, k % 2)
                grads_in(ahead, (k + 1) % 2, half, kept)
                in_grads(i, k % 2)
            return 0

        def chunk(c, _):
            lax.fori_loop(c * bodies, (c + 1) * bodies, body, 0)
            for m in range(3):
                terms[c, m] = acc[m].astype(BF)
                acc[m] = jnp.zeros_like(acc[m])
            return 0

        lax.fori_loop(0, chunks, chunk, 0)
        for copy in pending:
            copy.wait()
        for copy in first_tile if not turn else ():
            copy.start()

        def inputs(j, _):
            choose(j, {at - loop: steps for at, steps in table.items() if loop <= at < loop + BODIES}, reduce)
            io_in(src, j).wait()
            for k in range(2):
                rows = aligned(j * big + k * tm, tm)
                da = sum(dot_nt(g[c, rows, m * fc : (m + 1) * fc], w[l, c, m]) for c in range(chunks) for m in range(2))
                da = da.astype(BF).astype(F32)
                wide = io[j % 2, pl.ds(k * tm, tm), :].astype(F32)
                scale = scale_of(wide)
                along = jnp.mean(da * wide, -1, keepdims=True) * (scale * scale * scale)
                dh = (da * scale - wide * along).astype(BF).astype(F32)
                y[rows, :] = (y[rows, :].astype(F32) + dh).astype(BF)
            pl.when(j + 2 < BODIES)(lambda: io_in(src, j + 2).start())
            if l == 0:
                rows = aligned(j * big, big)
                pltpu.make_async_copy(y.at[rows, :], dx_hbm.at[rows, :], sem.at[0]).start()
            return 0

        lax.fori_loop(0, BODIES, inputs, 0)

    for m in range(3):
        acc[m] = jnp.zeros_like(acc[m])
    first_tile = [pltpu.make_async_copy(gu_hbm.at[0, m], acc.at[0, pl.ds(m * tm, tm), :], gu_sem.at[m]) for m in range(2)]

    def with_last(a2, out):
        def io_out(j):
            return pltpu.make_async_copy(out.at[j % 2], h_hbm.at[aligned(j * big, big), :], io_sem.at[1, j % 2])

        def down(j, _):
            choose(j, GATHER_DOWN, gather)
            pl.when(j == 0)(lambda: arrived(2 * chunks))
            io_in(x_hbm, j).wait()
            pl.when(j >= 2)(lambda: io_out(j - 2).wait())
            for k in range(2):
                rows = aligned(j * big + k * tm, tm)
                hidden = sum(dot(g[c, rows, :fc], w[0, c, 2]) for c in range(chunks))
                here = pl.ds(k * tm, tm)
                h = (io[j % 2, here, :].astype(F32) + hidden.astype(BF).astype(F32)).astype(BF)
                out[j % 2, here, :] = h
                a2[rows, :] = normed(h.astype(F32))
            io_out(j).start()
            pl.when(j + 2 < BODIES)(lambda: io_in(x_hbm, j + 2).start())
            return 0

        lax.fori_loop(0, BODIES, down, 0)
        load_dy.wait()
        arrived(2 * chunks + 1)
        backward(0, a2, None, 0, [io_out(BODIES - 2), io_out(BODIES - 1)])

    pl.run_scoped(with_last, pltpu.VMEM((tokens, d), BF), pltpu.VMEM((2, big, d), BF))

    def with_first(gate_up):
        backward(1, a1, gate_up, chunks * TILES // WIDTHS[0] + BODIES, ())

    pl.run_scoped(with_first, pltpu.VMEM((3, 2, 2, tm, fc), F32))

    reduce(SUMS[max(SUMS)])
    for p in range(chunks):
        down_out(0, p).wait()
    for m in range(2):
        for j in range(3):
            in_out(0, m, j).wait()
    pltpu.make_async_copy(y, dx_hbm, sem.at[0]).wait()
    for i in range(len(ITEMS)):
        ref = piece(i, pl.ds(0, (n - 1) * own))
        pltpu.make_async_copy(ref, ref, ag_send.at[i]).wait()


def layers_of(n, x, dy, gate, up, down):
    tokens, d = x.shape
    layers, own, ff = gate.shape
    fc = ff // CHUNKS
    tm = tokens // TILES
    items = 3 * CHUNKS + 1
    assert d == fc == n * own and down.shape == (layers, CHUNKS * own, d) and own == 64
    assert n == 8 and layers == 2
    hbm = pl.BlockSpec(memory_space=pl.ANY)
    dma = pltpu.SemaphoreType.DMA
    kept = jax.ShapeDtypeStruct((CHUNKS * TILES, 2, tm, fc), F32)
    return pl.pallas_call(
        functools.partial(kernel, n),
        out_shape=[*(jax.ShapeDtypeStruct(t.shape, BF) for t in (x, gate, up, down, x)), kept],
        in_specs=[hbm] * 5,
        out_specs=[hbm] * 6,
        scratch_shapes=[
            pltpu.VMEM((tokens, d), BF),
            pltpu.VMEM((tokens, d), BF),
            pltpu.VMEM((CHUNKS, tokens, 2 * fc), BF),
            pltpu.VMEM((layers, CHUNKS, 3, d, fc), BF),
            pltpu.VMEM((3, d, fc), F32),
            pltpu.VMEM((tm, fc), BF),
            pltpu.VMEM((tm, fc), BF),
            pltpu.VMEM((tm, 2 * fc), BF),
            pltpu.VMEM((tm, 2 * fc), BF),
            pltpu.VMEM((CHUNKS, 3, d, fc), BF),
            pltpu.VMEM((CHUNKS, 3, n - 1, own, fc), BF),
            pltpu.VMEM((CHUNKS, 3, own, fc), BF),
            pltpu.VMEM((2, 2 * tm, d), BF),
            dma((2 + layers * 9,)),
            dma((2, 2)),
            dma((3,)),
            dma((CHUNKS * 3,)),
            dma((items, n - 1)),
            dma((items,)),
            dma((items,)),
            dma((CHUNKS, 3, n - 1)),
            dma((CHUNKS, 3)),
            pltpu.SemaphoreType.REGULAR((2, CHUNKS, 3)),
        ],
        compiler_params=pltpu.CompilerParams(vmem_limit_bytes=VMEM_LIMIT, has_side_effects=True, collective_id=0),
        name="layers",
    )(x, dy, gate, up, down)[:4]


def copied(*arrays):
    parts = [t.reshape(-1, t.shape[-1]) for t in arrays]
    cuts = [8, *(1 for _ in parts[1:])]

    def kernel(*refs):
        k = len(parts)
        src, dst, bufs, sems = refs[:k], refs[k : 2 * k], refs[2 * k : 3 * k], refs[3 * k]
        moves = []
        for which, (s, t, buf, cut) in enumerate(zip(src, dst, bufs, cuts)):
            size = s.shape[0] // cut
            for j in range(cut):
                rows = pl.ds(j * size, size)
                at = sems.at[:, 8 * which + j]
                moves.append((pltpu.make_async_copy(s.at[rows], buf.at[rows], at.at[0]), pltpu.make_async_copy(buf.at[rows], t.at[rows], at.at[1])))
        for there, _ in moves:
            there.start()
        for there, back in moves:
            there.wait()
            back.start()
        for _, back in moves:
            back.wait()

    hbm = pl.BlockSpec(memory_space=pl.ANY)
    out = pl.pallas_call(
        kernel,
        out_shape=[jax.ShapeDtypeStruct(t.shape, t.dtype) for t in parts],
        in_specs=[hbm] * len(parts),
        out_specs=[hbm] * len(parts),
        scratch_shapes=[*(pltpu.VMEM(t.shape, t.dtype) for t in parts), pltpu.SemaphoreType.DMA((2, 8 * len(parts)))],
        name="outputs",
    )(*parts)
    return [t.reshape(like.shape) for t, like in zip(out, arrays)]


def solution(mesh):
    n = mesh.shape["dp"]
    assert mesh.shape["rep"] % 2 == 0

    def local(x, dy, gate, up, down):
        dx, *grads = copied(*layers_of(n, x[0], dy[0], gate, up, down))
        return dx[None], *grads

    both, rows = P(("rep", "dp"), None, None), P(None, "dp", None)
    grads = P("rep", "dp", None)
    return jax.shard_map(
        local, mesh=mesh, in_specs=(both, both, rows, rows, rows), out_specs=(both, grads, grads, grads), check_vma=False
    )
```

```python
import functools

import jax
import jax.numpy as jnp
from jax import lax
from jax.experimental import pallas as pl
from jax.experimental.pallas import tpu as pltpu
from jax.sharding import PartitionSpec as P

BF = jnp.bfloat16
F32 = jnp.float32
CHUNKS = 3
TILES = 16
BODIES = TILES // 2

GATHER_START = (
    ((0, 0), (1, 0), (2, 0), (3, 0), (4, 0), (5, 0)),
    ((0, 1), (1, 1), (3, 1), (4, 1), (5, 1)),
    ((0, 2), (1, 2), (2, 1), (6, 0)),
    ((0, 3), (1, 3), (2, 2), (3, 2), (5, 2), (6, 1)),
    ((0, 4), (1, 4), (2, 3), (3, 3)),
)
GATHER_HIDDEN = {
    0: ((4, 2),), 2: ((7, 0),), 4: ((6, 2),), 5: ((3, 4), (5, 3)), 6: ((2, 4),), 7: ((4, 3),), 8: ((7, 1),), 11: ((6, 3), (8, 0)),
    12: ((9, 0),), 13: ((5, 4),), 14: ((4, 4),), 16: ((7, 2),), 21: ((6, 4), (8, 1)), 22: ((9, 1),),
}
GATHER_DOWN = {1: ((7, 3),), 4: ((8, 2),), 6: ((7, 4),), 7: ((9, 2),)}
GATHER_BACK = {0: ((8, 3),), 2: ((8, 4), (9, 3)), 4: ((9, 4),)}
WIDTHS = (4, 2)

SUMS = {
    4: ((0, 0, 0, 0),), 6: ((0, 0, 1, 0), (0, 0, 2, 0),), 7: ((0, 0, 0, 1),), 8: ((0, 1, 0, 0), (0, 1, 2, 0),),
    10: ((0, 0, 1, 1), (0, 0, 2, 1), (0, 1, 0, 1), (0, 1, 2, 1),), 11: ((0, 1, 1, 0),), 12: ((0, 0, 1, 2), (0, 0, 2, 2),), 13: ((0, 2, 1, 0),),
    14: ((0, 1, 1, 1), (0, 2, 0, 0), (0, 2, 2, 0),), 15: ((0, 0, 2, 3), (0, 0, 0, 2), (0, 1, 2, 2),), 16: ((0, 1, 0, 2), (0, 2, 1, 1),),
    18: ((0, 0, 2, 4), (0, 2, 0, 1),), 19: ((0, 2, 2, 1),), 20: ((0, 0, 0, 3),), 21: ((0, 1, 1, 2),), 22: ((0, 1, 0, 3), (0, 2, 0, 2),),
    23: ((0, 0, 0, 4), (0, 0, 1, 3), (0, 2, 1, 2), (0, 2, 2, 2),), 25: ((0, 1, 0, 4), (0, 1, 1, 3),), 26: ((0, 1, 2, 3),),
    27: ((0, 0, 1, 4), (0, 2, 0, 3),), 28: ((0, 1, 1, 4), (1, 0, 2, 0),), 29: ((1, 0, 0, 0),), 30: ((0, 1, 2, 4), (0, 2, 0, 4), (1, 0, 1, 0),),
    31: ((1, 0, 2, 1),), 32: ((1, 0, 0, 1),), 33: ((1, 0, 1, 1),), 34: ((0, 2, 2, 3), (1, 0, 2, 2),), 35: ((1, 0, 0, 2),),
    36: ((1, 0, 1, 2), (1, 1, 0, 0),), 37: ((0, 2, 2, 4),), 38: ((0, 2, 1, 3), (1, 1, 1, 0), (1, 1, 2, 0),), 39: ((1, 0, 0, 3), (1, 0, 2, 3),),
    40: ((1, 0, 1, 3),), 41: ((0, 2, 1, 4), (1, 1, 0, 1),), 42: ((1, 1, 1, 1),), 43: ((1, 0, 0, 4), (1, 1, 2, 1),),
    44: ((1, 0, 1, 4), (1, 0, 2, 4), (1, 2, 0, 0), (1, 2, 1, 0),), 45: ((1, 1, 0, 2), (1, 2, 2, 0),), 46: ((1, 1, 2, 2),),
    47: ((1, 2, 0, 1), (1, 2, 1, 1),), 48: ((1, 2, 2, 1),), 49: ((1, 1, 1, 2), (1, 2, 0, 2),), 50: ((1, 2, 1, 2), (1, 2, 2, 2),),
    51: ((1, 1, 0, 3), (1, 1, 1, 3), (1, 1, 2, 3), (1, 2, 0, 3),),
    52: ((1, 2, 1, 3), (1, 2, 2, 3), (1, 1, 0, 4), (1, 1, 1, 4), (1, 1, 2, 4), (1, 2, 0, 4), (1, 2, 1, 4), (1, 2, 2, 4),),
}
EPS = 1e-6
VMEM_LIMIT = 67043328


def dot(a, b):
    return lax.dot_general(a, b, (((1,), (0,)), ((), ())), preferred_element_type=F32)


def dot_nt(a, b):
    return lax.dot_general(a, b, (((1,), (1,)), ((), ())), preferred_element_type=F32)


def dot_tn(a, b):
    return lax.dot_general(a, b, (((0,), (0,)), ((), ())), preferred_element_type=F32)


def sigmoid(g):
    return 0.5 * jnp.tanh(0.5 * g) + 0.5


def scale_of(wide):
    return lax.rsqrt(jnp.mean(wide * wide, -1, keepdims=True) + EPS)


def normed(wide):
    return (wide * scale_of(wide)).astype(BF)


def aligned(start, size):
    return pl.ds(pl.multiple_of(start, size), size)


def choose(j, table, do):
    keys = sorted(table)
    if len(keys) == 1:
        pl.when(j == keys[0])(lambda: do(table[keys[0]]))
    elif keys:
        mid = keys[len(keys) // 2]
        pl.when(j < mid)(lambda: choose(j, {k: v for k, v in table.items() if k < mid}, do))
        pl.when(j >= mid)(lambda: choose(j, {k: v for k, v in table.items() if k >= mid}, do))


def kernel(
    n, x_hbm, dy_hbm, gate_hbm, up_hbm, down_hbm, y, dgate_hbm, dup_hbm, ddown_hbm, h_hbm, gu_hbm,
    a1, g, w, acc, act0, act1, g0, g1, terms, slots, fin, io,
    sem, io_sem, gu_sem, out_sem, ag_recv, ag_send, side_recv, rs_recv, rs_send, credit,
):
    layers, chunks = w.shape[:2]
    tokens, d = y.shape
    fc = w.shape[-1]
    own = d // n
    half = fc // 2
    tm = tokens // TILES
    big = 2 * tm
    acts, gs = (act0, act1), (g0, g1)
    near = (n - 1) // 2

    me = lax.axis_index("dp")
    core = lax.axis_index("rep") % 2
    left, right = {"dp": (me + n - 1) % n}, {"dp": (me + 1) % n}
    partner = {"rep": lax.axis_index("rep") + 1 - 2 * core}
    owner = [(me + k) % n * own for k in range(n)]

    def remote(src, dst, send, recv, to):
        return pltpu.make_async_remote_copy(src, dst, send, recv, device_id=to, device_id_type=pl.DeviceIdType.MESH)

    ITEMS = [(0, c, m) for c in range(chunks) for m in range(2)] + [(0, slice(None), 2)] + [(l, c, slice(None)) for l in range(1, layers) for c in range(chunks)]

    def piece(i, rows):
        return w.at[(*ITEMS[i], rows, slice(None))]

    def gather(steps):
        with jax.named_scope("gather"):
            for i, h in steps:
                far = near + i % 2
                for side, to in enumerate((right, left)):
                    reach = (far, n - 1 - far)[side]
                    if h > reach:
                        continue
                    ref = piece(i, aligned(owner[(n - h) % n if side == 0 else h] + core * (own // 2), own // 2))
                    at = side * far + h
                    if h:
                        remote(ref, ref, ag_send.at[i], ag_recv.at[i, at - 1], to).wait_recv()
                    if h < reach:
                        remote(ref, ref, ag_send.at[i], ag_recv.at[i, at], to).start()
                    if h:
                        remote(ref, ref, ag_send.at[i], side_recv.at[i], partner).start()

    def arrived(*which):
        with jax.named_scope("arrived"):
            for i in which:
                ref = piece(i, pl.ds(0, (n - 1) * (own // 2)))
                pltpu.make_async_copy(ref, ref, side_recv.at[i]).wait()

    def reduce(events):
        with jax.named_scope("sums"):
            for turn, p, u, s in events:
                far = near + (p + u) % 2
                for side, to in enumerate((right, left)):
                    reach = (far, n - 1 - far)[side]
                    if s >= reach:
                        continue
                    at = side * far + s
                    rows = aligned(owner[reach - s if side == 0 else n - reach + s], own)
                    if s == 0:
                        if turn:
                            pl.semaphore_wait(credit.at[side, p, u], 1)
                        ref = terms.at[p, u, rows, :]
                    else:
                        ref = slots.at[p, u, at - 1]
                        remote(ref, ref, rs_send.at[p, u], rs_recv.at[p, u, at - 1], to).wait_recv()
                        ref[...] = (ref[...].astype(F32) + terms[p, u, rows, :].astype(F32)).astype(BF)
                    remote(ref, slots.at[p, u, at], rs_send.at[p, u], rs_recv.at[p, u, at], to).start()
                if s == near + 1:
                    finish(turn, p, u, far)

    def down_out(l, p):
        return pltpu.make_async_copy(fin.at[p, 2], ddown_hbm.at[l, pl.ds(p * own, own), :], out_sem.at[p])

    def in_out(l, m, j):
        out = dgate_hbm if m == 0 else dup_hbm
        return pltpu.make_async_copy(fin.at[j, m], out.at[l, :, pl.ds(j * d, d)], out_sem.at[chunks + m * chunks + j])

    def finish(turn, p, u, far):
        l = layers - 1 - turn
        ends = [slots.at[p, u, far - 1], slots.at[p, u, n - 2]]
        for ref, at in zip(ends, (far - 1, n - 2)):
            remote(ref, ref, rs_send.at[p, u], rs_recv.at[p, u, at], right).wait_recv()
        if turn:
            (down_out(l + 1, p) if u == 2 else in_out(l + 1, u, p)).wait()
        rows = aligned(owner[0], own)
        fin[p, u] = (ends[0][...].astype(F32) + ends[1][...].astype(F32) + terms[p, u, rows, :].astype(F32)).astype(BF)
        ref = w.at[0, 0, 0, pl.ds(0, (n - 1) * own), :]
        pltpu.make_async_copy(ref, ref, rs_send.at[p, u]).wait()
        if l:
            pl.semaphore_signal(credit.at[0, p, u], 1, device_id=left, device_id_type=pl.DeviceIdType.MESH)
            pl.semaphore_signal(credit.at[1, p, u], 1, device_id=right, device_id_type=pl.DeviceIdType.MESH)
        if u == 2:
            down_out(l, p).start()
        if u < 2 and p == chunks - 1:
            low = lax.broadcasted_iota(jnp.int32, (own, 128), 1) < 64
            parts = [[fin[c, u, :, pl.ds(128 * e, 128)] for e in range(fc // 128)] for c in range(chunks)]
            for e in range(fc // 128):
                c0, c1, c2 = (parts[c][e].astype(F32) for c in range(chunks))
                c1 = pltpu.roll(c1, 64, 1)
                for k, (lo, hi) in enumerate(((c0, c1), (c2, c0), (c1, c2))):
                    j, at = divmod(3 * e + k, d // 128)
                    fin[j, u, :, pl.ds(128 * at, 128)] = jnp.where(low, lo, hi).astype(BF)
            for j in range(3):
                in_out(l, u, j).start()

    shards = (gate_hbm, up_hbm)
    raw = [
        pltpu.make_async_copy(shards[m].at[l, :, pl.ds(j * d, d)], terms.at[l, m, pl.ds(j * own, own), :], sem.at[2 + (l * 2 + m) * 3 + j])
        for l in range(layers) for m in range(2) for j in range(3)
    ]
    downs = [
        pltpu.make_async_copy(down_hbm.at[l, pl.ds(c * own, own), :], w.at[l, c, 2, aligned(owner[0], own), :], sem.at[2 + layers * 6 + l * 3 + c])
        for l in range(layers) for c in range(chunks)
    ]
    load_x, load_dy = pltpu.make_async_copy(x_hbm, a1, sem.at[0]), pltpu.make_async_copy(dy_hbm, y, sem.at[1])
    for copy in (*raw, *downs, load_x, load_dy):
        copy.start()
    barrier = pltpu.get_barrier_semaphore()
    for to in (left, right, partner):
        pl.semaphore_signal(barrier, 1, device_id=to, device_id_type=pl.DeviceIdType.MESH)
    with jax.named_scope("rawwait"):
        for copy in (*raw, *downs):
            copy.wait()
    low = lax.broadcasted_iota(jnp.int32, (own, 128), 1) < 64
    for l in range(layers):
        for m in range(2):
            for e in range(fc // 128):
                parts = []
                for k in range(3):
                    j, at = divmod(3 * e + k, d // 128)
                    parts.append(terms[l, m, pl.ds(j * own, own), pl.ds(128 * at, 128)].astype(F32))
                k0, k1, k2 = parts
                mixed = (jnp.where(low, k0, k1), pltpu.roll(jnp.where(low, k2, k0), 64, 1), jnp.where(low, k1, k2))
                for c in range(chunks):
                    w[l, c, m, aligned(owner[0], own), pl.ds(128 * e, 128)] = mixed[c].astype(BF)
    with jax.named_scope("barr"):
        pl.semaphore_wait(barrier, 3)

    gather(GATHER_START[0])
    load_x.wait()

    def norm_x(t, _):
        rows = aligned(t * tm, tm)
        a1[rows, :] = normed(a1[rows, :].astype(F32))
        return 0

    with jax.named_scope("norm"):
        lax.fori_loop(0, TILES, norm_x, 0)
    for steps in GATHER_START[1:]:
        gather(steps)
    arrived(0, 1)

    def hidden_units(keep):
        def keep_out(b):
            return pltpu.make_async_copy(keep.at[b % 3], gu_hbm.at[pl.ds(2 * b, 2)], gu_sem.at[b % 3])

        def body(b, _):
            choose(b, GATHER_HIDDEN, gather)
            choose(b, {BODIES * c: (2 * c, 2 * c + 1) for c in range(1, chunks)}, lambda which: arrived(*which))
            with jax.named_scope("keepwait"):
                pl.when(b >= 3)(lambda: keep_out(b - 3).wait())
            c = b // BODIES
            with jax.named_scope("hidden"):
                for k in range(2):
                    rows = aligned(b % BODIES * big + k * tm, tm)
                    at = a1[rows, :]
                    for f in (0, half):
                        gate = dot(at, w[0, c, 0, :, f : f + half])
                        up = dot(at, w[0, c, 1, :, f : f + half])
                        keep[b % 3, k, 0, :, f : f + half] = gate
                        keep[b % 3, k, 1, :, f : f + half] = up
                        g[c, rows, f : f + half] = (gate * sigmoid(gate) * up).astype(BF)
            keep_out(b).start()
            return 0

        lax.fori_loop(0, chunks * BODIES, body, 0)
        for b in range(chunks * BODIES - 3, chunks * BODIES):
            keep_out(b).wait()

    def io_in(src, j):
        return pltpu.make_async_copy(src.at[aligned(j * big, big), :], io.at[j % 2], io_sem.at[0, j % 2])

    io_in(x_hbm, 0).start()
    io_in(x_hbm, 1).start()
    pl.run_scoped(hidden_units, pltpu.VMEM((3, 2, 2, tm, fc), F32))

    def backward(turn, a, gate_up, start, pending):
        l = layers - 1 - turn
        width = WIDTHS[turn]
        bodies = TILES // width
        table = {at - start: steps for at, steps in SUMS.items() if at >= start}
        loop = chunks * bodies
        tiles = chunks * TILES

        def grads_in(i, slot, f, kept):
            c, t = i // TILES, i % TILES
            rows = aligned(t * tm, tm)
            if kept is None:
                at = a[rows, :]
                gate = dot(at, w[l, c, 0, :, f : f + half])
                up = dot(at, w[l, c, 1, :, f : f + half])
            else:
                gate, up = kept[0, :, f : f + half], kept[1, :, f : f + half]
            dact = dot_nt(y[rows, :], w[l, c, 2, f : f + half, :]).astype(BF).astype(F32)
            s = sigmoid(gate)
            silu = gate * s
            acts[slot][:, f : f + half] = (silu * up).astype(BF)
            dgate = (dact * up * (s + silu * (1.0 - s))).astype(BF)
            dup = (dact * silu).astype(BF)
            gs[slot][:, f : f + half] = dgate
            gs[slot][:, fc + f : fc + f + half] = dup
            g[c, rows, f : f + half] = dgate
            g[c, rows, fc + f : fc + f + half] = dup

        def down_grad(i, slot):
            rows = aligned(i % TILES * tm, tm)
            acc[2] += dot_tn(acts[slot][...], y[rows, :])

        def in_grads(i, slot):
            rows = aligned(i % TILES * tm, tm)
            at = a[rows, :]
            acc[0] += dot_tn(at, gs[slot][:, :fc])
            acc[1] += dot_tn(at, gs[slot][:, fc:])

        def first_of(j):
            return jnp.minimum(2 * j + 1, tiles - 2)

        def block_in(j):
            return pltpu.make_async_copy(gu_hbm.at[pl.ds(first_of(j), 2)], gate_up.at[j % 3], gu_sem.at[j % 3])

        src = h_hbm if l else x_hbm
        io_in(src, 0).start()
        io_in(src, 1).start()
        if turn:
            for copy in first_tile:
                copy.wait()
            block_in(0).start()
            block_in(1).start()
        with jax.named_scope("a0"):
            for f in (0, half):
                grads_in(0, 0, f, acc.at[0, pl.ds(0, 2 * tm), :].reshape(2, tm, fc) if turn else None)
            if turn:
                acc[0] = jnp.zeros_like(acc[0])

        def body(j, _):
            if not turn:
                choose(j, GATHER_BACK, gather)
                choose(j, {bodies * c - 1: 3 * chunks - 2 + c for c in range(1, chunks)}, lambda i: arrived(i))
            choose(j, {at: steps for at, steps in table.items() if at < loop}, reduce)
            if turn:
                with jax.named_scope("blkw"):
                    block_in(j).wait()
                pl.when(j + 2 < loop)(lambda: block_in(j + 2).start())
            with jax.named_scope("p1"):
                for k in range(width):
                    i = width * j + k
                    ahead = jnp.minimum(i + 1, tiles - 1)
                    kept = gate_up.at[j % 3, ahead - first_of(j) if k == 0 else 1] if turn else None
                    grads_in(ahead, (k + 1) % 2, 0, kept)
                    down_grad(i, k % 2)
                    grads_in(ahead, (k + 1) % 2, half, kept)
                    in_grads(i, k % 2)
            return 0

        def chunk(c, _):
            lax.fori_loop(c * bodies, (c + 1) * bodies, body, 0)
            with jax.named_scope("cend"):
                for m in range(3):
                    terms[c, m] = acc[m].astype(BF)
                    acc[m] = jnp.zeros_like(acc[m])
            return 0

        lax.fori_loop(0, chunks, chunk, 0)
        for copy in pending:
            copy.wait()
        for copy in first_tile if not turn else ():
            copy.start()

        def inputs(j, _):
            choose(j, {at - loop: steps for at, steps in table.items() if loop <= at < loop + BODIES}, reduce)
            with jax.named_scope("iow2"):
                io_in(src, j).wait()
            with jax.named_scope("p2"):
                for k in range(2):
                    rows = aligned(j * big + k * tm, tm)
                    da = sum(dot_nt(g[c, rows, m * fc : (m + 1) * fc], w[l, c, m]) for c in range(chunks) for m in range(2))
                    da = da.astype(BF).astype(F32)
                    wide = io[j % 2, pl.ds(k * tm, tm), :].astype(F32)
                    scale = scale_of(wide)
                    along = jnp.mean(da * wide, -1, keepdims=True) * (scale * scale * scale)
                    dh = (da * scale - wide * along).astype(BF).astype(F32)
                    y[rows, :] = (y[rows, :].astype(F32) + dh).astype(BF)
            pl.when(j + 2 < BODIES)(lambda: io_in(src, j + 2).start())
            return 0

        lax.fori_loop(0, BODIES, inputs, 0)

    for m in range(3):
        acc[m] = jnp.zeros_like(acc[m])
    first_tile = [pltpu.make_async_copy(gu_hbm.at[0, m], acc.at[0, pl.ds(m * tm, tm), :], gu_sem.at[m]) for m in range(2)]

    def with_last(a2, out):
        def io_out(j):
            return pltpu.make_async_copy(out.at[j % 2], h_hbm.at[aligned(j * big, big), :], io_sem.at[1, j % 2])

        def down(j, _):
            choose(j, GATHER_DOWN, gather)
            pl.when(j == 0)(lambda: arrived(2 * chunks))
            with jax.named_scope("iow"):
                io_in(x_hbm, j).wait()
            pl.when(j >= 2)(lambda: io_out(j - 2).wait())
            with jax.named_scope("down"):
                for k in range(4):
                    rows = aligned(j * big + k * (tm // 2), tm // 2)
                    hidden = sum(dot(g[c, rows, :fc], w[0, c, 2]) for c in range(chunks))
                    here = pl.ds(k * (tm // 2), tm // 2)
                    h = (io[j % 2, here, :].astype(F32) + hidden.astype(BF).astype(F32)).astype(BF)
                    out[j % 2, here, :] = h
                    a2[rows, :] = normed(h.astype(F32))
            io_out(j).start()
            pl.when(j + 2 < BODIES)(lambda: io_in(x_hbm, j + 2).start())
            return 0

        lax.fori_loop(0, BODIES, down, 0)
        load_dy.wait()
        arrived(2 * chunks + 1)
        backward(0, a2, None, 0, [io_out(BODIES - 2), io_out(BODIES - 1)])

    pl.run_scoped(with_last, pltpu.VMEM((tokens, d), BF), pltpu.VMEM((2, big, d), BF))

    def with_first(gate_up):
        backward(1, a1, gate_up, chunks * TILES // WIDTHS[0] + BODIES, ())

    pl.run_scoped(with_first, pltpu.VMEM((3, 2, 2, tm, fc), F32))

    reduce(SUMS[max(SUMS)])
    with jax.named_scope("ends"):
        for p in range(chunks):
            down_out(0, p).wait()
        for m in range(2):
            for j in range(3):
                in_out(0, m, j).wait()
        for i in range(len(ITEMS)):
            ref = piece(i, pl.ds(0, (n - 1) * own))
            pltpu.make_async_copy(ref, ref, ag_send.at[i]).wait()


def layers_of(n, x, dy, gate, up, down):
    tokens, d = x.shape
    layers, own, ff = gate.shape
    fc = ff // CHUNKS
    tm = tokens // TILES
    items = 3 * CHUNKS + 1
    assert d == fc == n * own and down.shape == (layers, CHUNKS * own, d) and own == 64
    assert n == 8 and layers == 2
    hbm, vmem = pl.BlockSpec(memory_space=pl.ANY), pl.BlockSpec(memory_space=pltpu.VMEM)
    dma = pltpu.SemaphoreType.DMA
    kept = jax.ShapeDtypeStruct((CHUNKS * TILES, 2, tm, fc), F32)
    return pl.pallas_call(
        functools.partial(kernel, n),
        out_shape=[pltpu.VMEM((tokens, d), BF), *(jax.ShapeDtypeStruct(t.shape, BF) for t in (gate, up, down, x)), kept],
        in_specs=[hbm] * 5,
        out_specs=[vmem] + [hbm] * 5,
        scratch_shapes=[
            pltpu.VMEM((tokens, d), BF),
            pltpu.VMEM((CHUNKS, tokens, 2 * fc), BF),
            pltpu.VMEM((layers, CHUNKS, 3, d, fc), BF),
            pltpu.VMEM((3, d, fc), F32),
            pltpu.VMEM((tm, fc), BF),
            pltpu.VMEM((tm, fc), BF),
            pltpu.VMEM((tm, 2 * fc), BF),
            pltpu.VMEM((tm, 2 * fc), BF),
            pltpu.VMEM((CHUNKS, 3, d, fc), BF),
            pltpu.VMEM((CHUNKS, 3, n - 1, own, fc), BF),
            pltpu.VMEM((CHUNKS, 3, own, fc), BF),
            pltpu.VMEM((2, 2 * tm, d), BF),
            dma((2 + layers * 9,)),
            dma((2, 2)),
            dma((3,)),
            dma((CHUNKS * 3,)),
            dma((items, n - 1)),
            dma((items,)),
            dma((items,)),
            dma((CHUNKS, 3, n - 1)),
            dma((CHUNKS, 3)),
            pltpu.SemaphoreType.REGULAR((2, CHUNKS, 3)),
        ],
        compiler_params=pltpu.CompilerParams(vmem_limit_bytes=VMEM_LIMIT - tokens * d * 2, has_side_effects=True, collective_id=0),
        name="layers",
    )(x, dy, gate, up, down)[:4]


def outputs(dx, *grads):
    parts = [t.reshape(-1, t.shape[-1]) for t in grads]

    def kernel(dx_ref, *refs):
        k = len(parts)
        src, dx_out, dst, bufs, sems = refs[:k], refs[k], refs[k + 1 : 2 * k + 1], refs[2 * k + 1 : 3 * k + 1], refs[3 * k + 1]
        ins = [pltpu.make_async_copy(s, buf, sems.at[0, j]) for j, (s, buf) in enumerate(zip(src, bufs))]
        outs = [pltpu.make_async_copy(buf, t, sems.at[1, j]) for j, (buf, t) in enumerate(zip(bufs, dst))]
        for copy in ins:
            copy.start()
        outs.append(pltpu.make_async_copy(dx_ref, dx_out, sems.at[0, k]))
        outs[-1].start()
        for there, back in zip(ins, outs):
            there.wait()
            back.start()
        for copy in outs:
            copy.wait()

    hbm, vmem = pl.BlockSpec(memory_space=pl.ANY), pl.BlockSpec(memory_space=pltpu.VMEM)
    out = pl.pallas_call(
        kernel,
        out_shape=[jax.ShapeDtypeStruct(t.shape, BF) for t in (dx, *parts)],
        in_specs=[vmem] + [hbm] * len(parts),
        out_specs=[hbm] * (1 + len(parts)),
        scratch_shapes=[*(pltpu.VMEM(t.shape, BF) for t in parts), pltpu.SemaphoreType.DMA((2, 1 + len(parts)))],
        compiler_params=pltpu.CompilerParams(vmem_limit_bytes=VMEM_LIMIT - dx.size * 2),
        name="outputs",
    )(pltpu.with_memory_space_constraint(dx, pltpu.VMEM), *parts)
    return [t.reshape(like.shape) for t, like in zip(out, (dx, *grads))]


def solution(mesh):
    n = mesh.shape["dp"]
    assert mesh.shape["rep"] % 2 == 0

    def local(x, dy, gate, up, down):
        dx, *grads = outputs(*layers_of(n, x[0], dy[0], gate, up, down))
        return dx[None], *grads

    both, rows = P(("rep", "dp"), None, None), P(None, "dp", None)
    grads = P("rep", "dp", None)
    return jax.shard_map(
        local, mesh=mesh, in_specs=(both, both, rows, rows, rows), out_specs=(both, grads, grads, grads), check_vma=False
    )
```

```python
import functools

import jax
import jax.numpy as jnp
from jax import lax
from jax.experimental import pallas as pl
from jax.experimental.pallas import tpu as pltpu
from jax.sharding import PartitionSpec as P

BF = jnp.bfloat16
F32 = jnp.float32
CHUNKS = 3
TILES = 16
BODIES = TILES // 2

GATHER_START = (
    ((0, 0), (1, 0), (2, 0), (3, 0), (4, 0), (5, 0)),
    ((0, 1), (1, 1), (3, 1), (4, 1), (5, 1)),
    ((0, 2), (1, 2), (2, 1), (6, 0)),
    ((0, 3), (1, 3), (2, 2), (3, 2), (5, 2), (6, 1)),
    ((0, 4), (1, 4), (2, 3), (3, 3)),
)
GATHER_HIDDEN = {
    0: ((4, 2),), 2: ((7, 0),), 4: ((6, 2),), 5: ((3, 4), (5, 3)), 6: ((2, 4),), 7: ((4, 3),), 8: ((7, 1),), 11: ((6, 3), (8, 0)),
    12: ((9, 0),), 13: ((5, 4),), 14: ((4, 4),), 16: ((7, 2),), 21: ((6, 4), (8, 1)), 22: ((9, 1),),
}
GATHER_DOWN = {1: ((7, 3),), 4: ((8, 2),), 6: ((7, 4),), 7: ((9, 2),)}
GATHER_BACK = {0: ((8, 3),), 2: ((8, 4), (9, 3)), 4: ((9, 4),)}
WIDTHS = (4, 2)

SUMS = {
    4: ((0, 0, 0, 0), (0, 0, 1, 0), (0, 0, 2, 0),), 6: ((0, 0, 0, 1), (0, 0, 1, 1), (0, 0, 2, 1),),
    8: ((0, 0, 1, 2), (0, 1, 0, 0), (0, 1, 1, 0), (0, 1, 2, 0),), 9: ((0, 0, 0, 2), (0, 0, 2, 2),), 10: ((0, 0, 1, 3), (0, 1, 0, 1), (0, 1, 1, 1),),
    11: ((0, 0, 0, 3), (0, 1, 2, 1),), 12: ((0, 0, 1, 4), (0, 2, 0, 0), (0, 2, 1, 0), (0, 2, 2, 0),),
    13: ((0, 0, 0, 4), (0, 0, 2, 3), (0, 1, 0, 2), (0, 1, 1, 2), (0, 1, 2, 2),), 14: ((0, 2, 0, 1),),
    16: ((0, 0, 2, 4), (0, 1, 0, 3), (0, 2, 1, 1), (0, 2, 2, 1),), 18: ((0, 1, 1, 3), (0, 1, 2, 3),), 19: ((0, 1, 0, 4), (0, 2, 0, 2),),
    20: ((0, 1, 1, 4), (0, 1, 2, 4), (0, 2, 1, 2), (0, 2, 2, 2),), 21: ((0, 2, 0, 3),), 25: ((0, 2, 0, 4),), 28: ((1, 0, 0, 0), (1, 0, 2, 0),),
    29: ((1, 0, 1, 0),), 31: ((1, 0, 0, 1),), 32: ((1, 0, 2, 1),), 33: ((0, 2, 2, 3), (1, 0, 1, 1),), 34: ((0, 2, 1, 3), (1, 0, 0, 2),),
    35: ((1, 0, 2, 2),), 36: ((0, 2, 2, 4), (1, 1, 0, 0), (1, 1, 2, 0),), 37: ((0, 2, 1, 4), (1, 0, 1, 2),), 38: ((1, 1, 1, 0),), 39: ((1, 0, 0, 3),),
    40: ((1, 1, 0, 1),), 41: ((1, 1, 2, 1),), 42: ((1, 0, 1, 3), (1, 0, 2, 3), (1, 1, 1, 1),), 43: ((1, 0, 0, 4),),
    44: ((1, 2, 0, 0), (1, 2, 1, 0), (1, 2, 2, 0),), 45: ((1, 0, 1, 4), (1, 0, 2, 4), (1, 1, 0, 2),), 46: ((1, 2, 0, 1),),
    47: ((1, 2, 1, 1), (1, 2, 2, 1),), 48: ((1, 1, 1, 2), (1, 1, 2, 2), (1, 2, 0, 2),), 49: ((1, 2, 1, 2),), 50: ((1, 2, 2, 2),),
    51: ((1, 1, 0, 3), (1, 1, 1, 3), (1, 1, 2, 3), (1, 2, 0, 3),),
    52: ((1, 2, 1, 3), (1, 2, 2, 3), (1, 1, 0, 4), (1, 1, 1, 4), (1, 1, 2, 4), (1, 2, 0, 4), (1, 2, 1, 4), (1, 2, 2, 4),),
}
EPS = 1e-6
VMEM_LIMIT = 67043328


def dot(a, b):
    return lax.dot_general(a, b, (((1,), (0,)), ((), ())), preferred_element_type=F32)


def dot_nt(a, b):
    return lax.dot_general(a, b, (((1,), (1,)), ((), ())), preferred_element_type=F32)


def dot_tn(a, b):
    return lax.dot_general(a, b, (((0,), (0,)), ((), ())), preferred_element_type=F32)


def sigmoid(g):
    return 0.5 * jnp.tanh(0.5 * g) + 0.5


def scale_of(wide):
    return lax.rsqrt(jnp.mean(wide * wide, -1, keepdims=True) + EPS)


def normed(wide):
    return (wide * scale_of(wide)).astype(BF)


def aligned(start, size):
    return pl.ds(pl.multiple_of(start, size), size)


def choose(j, table, do):
    keys = sorted(table)
    if len(keys) == 1:
        pl.when(j == keys[0])(lambda: do(table[keys[0]]))
    elif keys:
        mid = keys[len(keys) // 2]
        pl.when(j < mid)(lambda: choose(j, {k: v for k, v in table.items() if k < mid}, do))
        pl.when(j >= mid)(lambda: choose(j, {k: v for k, v in table.items() if k >= mid}, do))


def kernel(
    n, x_hbm, dy_hbm, gate_hbm, up_hbm, down_hbm, y, fin, dgate_hbm, dup_hbm, ddown_hbm, h_hbm, gu_hbm,
    a1, g, w, acc, act0, act1, g0, g1, terms, slots, io,
    sem, io_sem, gu_sem, first_sem, out_sem, ag_recv, ag_send, side_recv, rs_recv, rs_send, credit,
):
    layers, chunks = w.shape[:2]
    tokens, d = y.shape
    fc = w.shape[-1]
    own = d // n
    half = fc // 2
    tm = tokens // TILES
    big = 2 * tm
    acts, gs = (act0, act1), (g0, g1)
    near = (n - 1) // 2

    me = lax.axis_index("dp")
    core = lax.axis_index("rep") % 2
    left, right = {"dp": (me + n - 1) % n}, {"dp": (me + 1) % n}
    partner = {"rep": lax.axis_index("rep") + 1 - 2 * core}
    owner = [(me + k) % n * own for k in range(n)]

    def remote(src, dst, send, recv, to):
        return pltpu.make_async_remote_copy(src, dst, send, recv, device_id=to, device_id_type=pl.DeviceIdType.MESH)

    ITEMS = [(0, c, m) for c in range(chunks) for m in range(2)] + [(0, slice(None), 2)] + [(l, c, slice(None)) for l in range(1, layers) for c in range(chunks)]

    def piece(i, rows):
        return w.at[(*ITEMS[i], rows, slice(None))]

    def gather(steps):
        with jax.named_scope("gather"):
            for i, h in steps:
                far = near + i % 2
                for side, to in enumerate((right, left)):
                    reach = (far, n - 1 - far)[side]
                    if h > reach:
                        continue
                    ref = piece(i, aligned(owner[(n - h) % n if side == 0 else h] + core * (own // 2), own // 2))
                    at = side * far + h
                    if h:
                        remote(ref, ref, ag_send.at[i], ag_recv.at[i, at - 1], to).wait_recv()
                    if h < reach:
                        remote(ref, ref, ag_send.at[i], ag_recv.at[i, at], to).start()
                    if h:
                        remote(ref, ref, ag_send.at[i], side_recv.at[i], partner).start()

    def arrived(*which):
        with jax.named_scope("arrived"):
            for i in which:
                ref = piece(i, pl.ds(0, (n - 1) * (own // 2)))
                pltpu.make_async_copy(ref, ref, side_recv.at[i]).wait()

    def reduce(events):
        with jax.named_scope("sums"):
            for turn, p, u, s in events:
                far = near + (p + u) % 2
                for side, to in enumerate((right, left)):
                    reach = (far, n - 1 - far)[side]
                    if s >= reach:
                        continue
                    at = side * far + s
                    rows = aligned(owner[reach - s if side == 0 else n - reach + s], own)
                    if s == 0:
                        if turn:
                            pl.semaphore_wait(credit.at[side, p, u], 1)
                        ref = terms.at[p, u, rows, :]
                    else:
                        ref = slots.at[p, u, at - 1]
                        remote(ref, ref, rs_send.at[p, u], rs_recv.at[p, u, at - 1], to).wait_recv()
                        ref[...] = (ref[...].astype(F32) + terms[p, u, rows, :].astype(F32)).astype(BF)
                    remote(ref, slots.at[p, u, at], rs_send.at[p, u], rs_recv.at[p, u, at], to).start()
                if s == near + 1:
                    finish(turn, p, u, far)

    def down_out(l, p):
        return pltpu.make_async_copy(fin.at[p, 2], ddown_hbm.at[l - 1, pl.ds(p * own, own), :], out_sem.at[p])

    def in_out(l, m, j):
        out = dgate_hbm if m == 0 else dup_hbm
        return pltpu.make_async_copy(fin.at[j, m], out.at[l - 1, :, pl.ds(j * d, d)], out_sem.at[chunks + m * chunks + j])

    def finish(turn, p, u, far):
        l = layers - 1 - turn
        ends = [slots.at[p, u, far - 1], slots.at[p, u, n - 2]]
        for ref, at in zip(ends, (far - 1, n - 2)):
            remote(ref, ref, rs_send.at[p, u], rs_recv.at[p, u, at], right).wait_recv()
        if turn:
            (down_out(l + 1, p) if u == 2 else in_out(l + 1, u, p)).wait()
        rows = aligned(owner[0], own)
        fin[p, u] = (ends[0][...].astype(F32) + ends[1][...].astype(F32) + terms[p, u, rows, :].astype(F32)).astype(BF)
        ref = w.at[0, 0, 0, pl.ds(0, (n - 1) * own), :]
        pltpu.make_async_copy(ref, ref, rs_send.at[p, u]).wait()
        if l:
            pl.semaphore_signal(credit.at[0, p, u], 1, device_id=left, device_id_type=pl.DeviceIdType.MESH)
            pl.semaphore_signal(credit.at[1, p, u], 1, device_id=right, device_id_type=pl.DeviceIdType.MESH)
        if u == 2 and l:
            down_out(l, p).start()
        if u < 2 and p == chunks - 1:
            low = lax.broadcasted_iota(jnp.int32, (own, 128), 1) < 64
            parts = [[fin[c, u, :, pl.ds(128 * e, 128)] for e in range(fc // 128)] for c in range(chunks)]
            for e in range(fc // 128):
                c0, c1, c2 = (parts[c][e].astype(F32) for c in range(chunks))
                c1 = pltpu.roll(c1, 64, 1)
                for k, (lo, hi) in enumerate(((c0, c1), (c2, c0), (c1, c2))):
                    j, at = divmod(3 * e + k, d // 128)
                    fin[j, u, :, pl.ds(128 * at, 128)] = jnp.where(low, lo, hi).astype(BF)
            for j in range(3) if l else ():
                in_out(l, u, j).start()

    shards = (gate_hbm, up_hbm)
    raw = [
        pltpu.make_async_copy(shards[m].at[l, :, pl.ds(j * d, d)], terms.at[l, m, pl.ds(j * own, own), :], sem.at[2 + (l * 2 + m) * 3 + j])
        for l in range(layers) for m in range(2) for j in range(3)
    ]
    downs = [
        pltpu.make_async_copy(down_hbm.at[l, pl.ds(c * own, own), :], w.at[l, c, 2, aligned(owner[0], own), :], sem.at[2 + layers * 6 + l * 3 + c])
        for l in range(layers) for c in range(chunks)
    ]
    load_x, load_dy = pltpu.make_async_copy(x_hbm, a1, sem.at[0]), pltpu.make_async_copy(dy_hbm, y, sem.at[1])
    for copy in (*raw, *downs, load_x, load_dy):
        copy.start()
    barrier = pltpu.get_barrier_semaphore()
    for to in (left, right, partner):
        pl.semaphore_signal(barrier, 1, device_id=to, device_id_type=pl.DeviceIdType.MESH)
    with jax.named_scope("rawwait"):
        for copy in (*raw, *downs):
            copy.wait()
    low = lax.broadcasted_iota(jnp.int32, (own, 128), 1) < 64
    for l in range(layers):
        for m in range(2):
            for e in range(fc // 128):
                parts = []
                for k in range(3):
                    j, at = divmod(3 * e + k, d // 128)
                    parts.append(terms[l, m, pl.ds(j * own, own), pl.ds(128 * at, 128)].astype(F32))
                k0, k1, k2 = parts
                mixed = (jnp.where(low, k0, k1), pltpu.roll(jnp.where(low, k2, k0), 64, 1), jnp.where(low, k1, k2))
                for c in range(chunks):
                    w[l, c, m, aligned(owner[0], own), pl.ds(128 * e, 128)] = mixed[c].astype(BF)
    with jax.named_scope("barr"):
        pl.semaphore_wait(barrier, 3)

    gather(GATHER_START[0])
    load_x.wait()

    def norm_x(t, _):
        rows = aligned(t * tm, tm)
        a1[rows, :] = normed(a1[rows, :].astype(F32))
        return 0

    with jax.named_scope("norm"):
        lax.fori_loop(0, TILES, norm_x, 0)
    for steps in GATHER_START[1:]:
        gather(steps)
    arrived(0, 1)

    def hidden_units(keep):
        def keep_out(b):
            return pltpu.make_async_copy(keep.at[b % 3], gu_hbm.at[pl.ds(2 * b, 2)], gu_sem.at[b % 3])

        def body(b, _):
            choose(b, GATHER_HIDDEN, gather)
            choose(b, {BODIES * c: (2 * c, 2 * c + 1) for c in range(1, chunks)}, lambda which: arrived(*which))
            with jax.named_scope("keepwait"):
                pl.when(b >= 3)(lambda: keep_out(b - 3).wait())
            c = b // BODIES
            with jax.named_scope("hidden"):
                for k in range(2):
                    rows = aligned(b % BODIES * big + k * tm, tm)
                    at = a1[rows, :]
                    for f in (0, half):
                        gate = dot(at, w[0, c, 0, :, f : f + half])
                        up = dot(at, w[0, c, 1, :, f : f + half])
                        keep[b % 3, k, 0, :, f : f + half] = gate
                        keep[b % 3, k, 1, :, f : f + half] = up
                        g[c, rows, f : f + half] = (gate * sigmoid(gate) * up).astype(BF)
            keep_out(b).start()
            return 0

        lax.fori_loop(0, chunks * BODIES, body, 0)
        for b in range(chunks * BODIES - 3, chunks * BODIES):
            keep_out(b).wait()

    def io_in(src, j):
        return pltpu.make_async_copy(src.at[aligned(j * big, big), :], io.at[j % 2], io_sem.at[0, j % 2])

    io_in(x_hbm, 0).start()
    io_in(x_hbm, 1).start()
    pl.run_scoped(hidden_units, pltpu.VMEM((3, 2, 2, tm, fc), F32))

    def backward(turn, a, gate_up, start, pending):
        l = layers - 1 - turn
        width = WIDTHS[turn]
        bodies = TILES // width
        table = {at - start: steps for at, steps in SUMS.items() if at >= start}
        loop = chunks * bodies
        tiles = chunks * TILES

        def grads_in(i, slot, f, kept):
            c, t = i // TILES, i % TILES
            rows = aligned(t * tm, tm)
            if kept is None:
                at = a[rows, :]
                gate = dot(at, w[l, c, 0, :, f : f + half])
                up = dot(at, w[l, c, 1, :, f : f + half])
            else:
                gate, up = kept[0, :, f : f + half], kept[1, :, f : f + half]
            dact = dot_nt(y[rows, :], w[l, c, 2, f : f + half, :]).astype(BF).astype(F32)
            s = sigmoid(gate)
            silu = gate * s
            acts[slot][:, f : f + half] = (silu * up).astype(BF)
            dgate = (dact * up * (s + silu * (1.0 - s))).astype(BF)
            dup = (dact * silu).astype(BF)
            gs[slot][:, f : f + half] = dgate
            gs[slot][:, fc + f : fc + f + half] = dup
            g[c, rows, f : f + half] = dgate
            g[c, rows, fc + f : fc + f + half] = dup

        def down_grad(i, slot):
            rows = aligned(i % TILES * tm, tm)
            acc[2] += dot_tn(acts[slot][...], y[rows, :])

        def in_grads(i, slot):
            rows = aligned(i % TILES * tm, tm)
            at = a[rows, :]
            acc[0] += dot_tn(at, gs[slot][:, :fc])
            acc[1] += dot_tn(at, gs[slot][:, fc:])

        def first_of(j):
            return jnp.minimum(2 * j + 1, tiles - 2)

        def block_in(j):
            return pltpu.make_async_copy(gu_hbm.at[pl.ds(first_of(j), 2)], gate_up.at[j % 3], gu_sem.at[j % 3])

        src = h_hbm if l else x_hbm
        io_in(src, 0).start()
        io_in(src, 1).start()
        if turn:
            block_in(1).start()
            for copy in first_tiles:
                copy.wait()
            for k in range(2):
                for m in range(2):
                    gate_up[0, k, m] = acc[1 + k, pl.ds(m * tm, tm), :]
        with jax.named_scope("a0"):
            for f in (0, half):
                grads_in(0, 0, f, acc.at[0].reshape(2, tm, fc) if turn else None)
            if turn:
                for m in range(3):
                    acc[m] = jnp.zeros_like(acc[m])

        def body(j, _):
            if not turn:
                choose(j, GATHER_BACK, gather)
                choose(j, {bodies * c - 1: 3 * chunks - 2 + c for c in range(1, chunks)}, lambda i: arrived(i))
            choose(j, {at: steps for at, steps in table.items() if at < loop}, reduce)
            if turn:
                pl.when(j > 0)(lambda: block_in(j).wait())
                pl.when(j + 2 < loop)(lambda: block_in(j + 2).start())
            with jax.named_scope("p1"):
                for k in range(width):
                    i = width * j + k
                    ahead = jnp.minimum(i + 1, tiles - 1)
                    kept = gate_up.at[j % 3, ahead - first_of(j) if k == 0 else 1] if turn else None
                    grads_in(ahead, (k + 1) % 2, 0, kept)
                    down_grad(i, k % 2)
                    grads_in(ahead, (k + 1) % 2, half, kept)
                    in_grads(i, k % 2)
            return 0

        def chunk(c, _):
            lax.fori_loop(c * bodies, (c + 1) * bodies, body, 0)
            with jax.named_scope("cend"):
                for m in range(3):
                    terms[c, m] = acc[m].astype(BF)
                    acc[m] = jnp.zeros_like(acc[m])
            return 0

        lax.fori_loop(0, chunks, chunk, 0)
        for copy in pending:
            copy.wait()
        for copy in first_tiles if not turn else ():
            copy.start()

        def inputs(j, _):
            choose(j, {at - loop: steps for at, steps in table.items() if loop <= at < loop + BODIES}, reduce)
            with jax.named_scope("iow2"):
                io_in(src, j).wait()
            with jax.named_scope("p2"):
                for k in range(2):
                    rows = aligned(j * big + k * tm, tm)
                    da = sum(dot_nt(g[c, rows, m * fc : (m + 1) * fc], w[l, c, m]) for c in range(chunks) for m in range(2))
                    da = da.astype(BF).astype(F32)
                    wide = io[j % 2, pl.ds(k * tm, tm), :].astype(F32)
                    scale = scale_of(wide)
                    along = jnp.mean(da * wide, -1, keepdims=True) * (scale * scale * scale)
                    dh = (da * scale - wide * along).astype(BF).astype(F32)
                    y[rows, :] = (y[rows, :].astype(F32) + dh).astype(BF)
            pl.when(j + 2 < BODIES)(lambda: io_in(src, j + 2).start())
            return 0

        lax.fori_loop(0, BODIES, inputs, 0)

    for m in range(3):
        acc[m] = jnp.zeros_like(acc[m])
    first_tiles = [pltpu.make_async_copy(gu_hbm.at[k, m], acc.at[k, pl.ds(m * tm, tm), :], first_sem.at[k, m]) for k in range(3) for m in range(2)]

    def with_last(a2, out):
        def io_out(j):
            return pltpu.make_async_copy(out.at[j % 2], h_hbm.at[aligned(j * big, big), :], io_sem.at[1, j % 2])

        def down(j, _):
            choose(j, GATHER_DOWN, gather)
            pl.when(j == 0)(lambda: arrived(2 * chunks))
            with jax.named_scope("iow"):
                io_in(x_hbm, j).wait()
            pl.when(j >= 2)(lambda: io_out(j - 2).wait())
            with jax.named_scope("down"):
                for k in range(4):
                    rows = aligned(j * big + k * (tm // 2), tm // 2)
                    hidden = sum(dot(g[c, rows, :fc], w[0, c, 2]) for c in range(chunks))
                    here = pl.ds(k * (tm // 2), tm // 2)
                    h = (io[j % 2, here, :].astype(F32) + hidden.astype(BF).astype(F32)).astype(BF)
                    out[j % 2, here, :] = h
                    a2[rows, :] = normed(h.astype(F32))
            io_out(j).start()
            pl.when(j + 2 < BODIES)(lambda: io_in(x_hbm, j + 2).start())
            return 0

        lax.fori_loop(0, BODIES, down, 0)
        load_dy.wait()
        arrived(2 * chunks + 1)
        backward(0, a2, None, 0, [io_out(BODIES - 2), io_out(BODIES - 1)])

    pl.run_scoped(with_last, pltpu.VMEM((tokens, d), BF), pltpu.VMEM((2, big, d), BF))

    def with_first(gate_up):
        backward(1, a1, gate_up, chunks * TILES // WIDTHS[0] + BODIES, ())

    pl.run_scoped(with_first, pltpu.VMEM((3, 2, 2, tm, fc), F32))

    reduce(SUMS[max(SUMS)])
    for i in range(len(ITEMS)):
        ref = piece(i, pl.ds(0, (n - 1) * own))
        pltpu.make_async_copy(ref, ref, ag_send.at[i]).wait()


def layers_of(n, x, dy, gate, up, down):
    tokens, d = x.shape
    layers, own, ff = gate.shape
    fc = ff // CHUNKS
    tm = tokens // TILES
    items = 3 * CHUNKS + 1
    assert d == fc == n * own and down.shape == (layers, CHUNKS * own, d) and own == 64
    assert n == 8 and layers == 2
    hbm, vmem = pl.BlockSpec(memory_space=pl.ANY), pl.BlockSpec(memory_space=pltpu.VMEM)
    dma = pltpu.SemaphoreType.DMA
    kept = jax.ShapeDtypeStruct((CHUNKS * TILES, 2, tm, fc), F32)
    return pl.pallas_call(
        functools.partial(kernel, n),
        out_shape=[
            pltpu.VMEM((tokens, d), BF),
            pltpu.VMEM((CHUNKS, 3, own, fc), BF),
            *(jax.ShapeDtypeStruct((layers - 1, *t.shape[1:]), BF) for t in (gate, up, down)),
            jax.ShapeDtypeStruct(x.shape, BF),
            kept,
        ],
        in_specs=[hbm] * 5,
        out_specs=[vmem] * 2 + [hbm] * 5,
        scratch_shapes=[
            pltpu.VMEM((tokens, d), BF),
            pltpu.VMEM((CHUNKS, tokens, 2 * fc), BF),
            pltpu.VMEM((layers, CHUNKS, 3, d, fc), BF),
            pltpu.VMEM((3, d, fc), F32),
            pltpu.VMEM((tm, fc), BF),
            pltpu.VMEM((tm, fc), BF),
            pltpu.VMEM((tm, 2 * fc), BF),
            pltpu.VMEM((tm, 2 * fc), BF),
            pltpu.VMEM((CHUNKS, 3, d, fc), BF),
            pltpu.VMEM((CHUNKS, 3, n - 1, own, fc), BF),
            pltpu.VMEM((2, 2 * tm, d), BF),
            dma((2 + layers * 9,)),
            dma((2, 2)),
            dma((3,)),
            dma((3, 2)),
            dma((CHUNKS * 3,)),
            dma((items, n - 1)),
            dma((items,)),
            dma((items,)),
            dma((CHUNKS, 3, n - 1)),
            dma((CHUNKS, 3)),
            pltpu.SemaphoreType.REGULAR((2, CHUNKS, 3)),
        ],
        compiler_params=pltpu.CompilerParams(vmem_limit_bytes=VMEM_LIMIT - (tokens * d + CHUNKS * 3 * own * fc) * 2, has_side_effects=True, collective_id=0),
        name="layers",
    )(x, dy, gate, up, down)[:5]


def outputs(layers, dx, first, *others):
    tokens, d = dx.shape
    chunks, _, own, fc = first.shape
    wide, tall = (layers, own, chunks * fc), (layers, chunks * own, d)

    def kernel(dx_ref, first_ref, gate_in, up_in, down_in, dx_out, gate_out, up_out, down_out, *rest):
        *bufs, sem, in_sem = rest
        grads = (gate_out, up_out, down_out)
        ins = [pltpu.make_async_copy(s, buf, in_sem.at[k]) for k, (s, buf) in enumerate(zip((gate_in, up_in, down_in), bufs))]
        moves = [pltpu.make_async_copy(dx_ref, dx_out, sem.at[0])]
        for m, out in enumerate(grads):
            for j in range(chunks):
                place = out.at[0, :, pl.ds(j * fc, fc)] if m < 2 else out.at[0, pl.ds(j * own, own), :]
                moves.append(pltpu.make_async_copy(first_ref.at[j, m], place, sem.at[1 + m * chunks + j]))
        for copy in (*ins, *moves):
            copy.start()
        for k, (copy, buf, out) in enumerate(zip(ins, bufs, grads)):
            copy.wait()
            moves.append(pltpu.make_async_copy(buf, out.at[pl.ds(1, layers - 1)], sem.at[1 + 3 * chunks + k]))
            moves[-1].start()
        for copy in moves:
            copy.wait()

    hbm, vmem = pl.BlockSpec(memory_space=pl.ANY), pl.BlockSpec(memory_space=pltpu.VMEM)
    kept = [pltpu.with_memory_space_constraint(t, pltpu.VMEM) for t in (dx, first)]
    return pl.pallas_call(
        kernel,
        out_shape=[jax.ShapeDtypeStruct(s, BF) for s in ((tokens, d), wide, wide, tall)],
        in_specs=[vmem] * 2 + [hbm] * 3,
        out_specs=[hbm] * 4,
        scratch_shapes=[*(pltpu.VMEM(t.shape, BF) for t in others), pltpu.SemaphoreType.DMA((4 + 3 * chunks,)), pltpu.SemaphoreType.DMA((3,))],
        compiler_params=pltpu.CompilerParams(vmem_limit_bytes=VMEM_LIMIT - (dx.size + first.size) * 2),
        name="outputs",
    )(*kept, *others)


def solution(mesh):
    n = mesh.shape["dp"]
    assert mesh.shape["rep"] % 2 == 0

    def local(x, dy, gate, up, down):
        dx, *grads = outputs(gate.shape[0], *layers_of(n, x[0], dy[0], gate, up, down))
        return dx[None], *grads

    both, rows = P(("rep", "dp"), None, None), P(None, "dp", None)
    grads = P("rep", "dp", None)
    return jax.shard_map(
        local, mesh=mesh, in_specs=(both, both, rows, rows, rows), out_specs=(both, grads, grads, grads), check_vma=False
    )
```

```python
import functools

import jax
import jax.numpy as jnp
from jax import lax
from jax.experimental import pallas as pl
from jax.experimental.pallas import tpu as pltpu
from jax.sharding import PartitionSpec as P

BF = jnp.bfloat16
F32 = jnp.float32
CHUNKS = 3
TILES = 16
BODIES = TILES // 2

GATHER_START = (
    ((0, 0), (1, 0), (2, 0), (3, 0), (4, 0), (5, 0)),
    ((0, 1), (1, 1), (3, 1), (4, 1), (5, 1)),
    ((0, 2), (1, 2), (2, 1), (6, 0)),
    ((0, 3), (1, 3), (2, 2), (3, 2), (5, 2), (6, 1)),
    ((0, 4), (1, 4), (2, 3), (3, 3)),
)
GATHER_HIDDEN = {
    0: ((4, 2),), 2: ((7, 0),), 4: ((6, 2),), 5: ((3, 4), (5, 3)), 6: ((2, 4),), 7: ((4, 3),), 8: ((7, 1),), 11: ((6, 3), (8, 0)),
    12: ((9, 0),), 13: ((5, 4),), 14: ((4, 4),), 16: ((7, 2),), 21: ((6, 4), (8, 1)), 22: ((9, 1),),
}
GATHER_DOWN = {1: ((7, 3),), 4: ((8, 2),), 6: ((7, 4),), 7: ((9, 2),)}
GATHER_BACK = {0: ((8, 3),), 2: ((8, 4), (9, 3)), 4: ((9, 4),)}
WIDTHS = (4, 2)
ORDERS = ((0, 1, 2, 3, 4), (1, 0, 2, 3, 4))

SUMS = {
    4: ((0, 0, 0, 0), (0, 0, 1, 0), (0, 0, 2, 0),), 6: ((0, 0, 0, 1), (0, 0, 1, 1), (0, 0, 2, 1),),
    8: ((0, 0, 1, 2), (0, 1, 0, 0), (0, 1, 1, 0), (0, 1, 2, 0),), 9: ((0, 0, 0, 2), (0, 0, 2, 2),), 10: ((0, 0, 1, 3), (0, 1, 0, 1), (0, 1, 1, 1),),
    11: ((0, 0, 0, 3), (0, 1, 2, 1),), 12: ((0, 0, 1, 4), (0, 2, 0, 0), (0, 2, 1, 0), (0, 2, 2, 0),),
    13: ((0, 0, 0, 4), (0, 0, 2, 3), (0, 1, 0, 2), (0, 1, 1, 2), (0, 1, 2, 2),), 14: ((0, 2, 0, 1),),
    16: ((0, 0, 2, 4), (0, 1, 0, 3), (0, 2, 1, 1), (0, 2, 2, 1),), 18: ((0, 1, 1, 3), (0, 1, 2, 3),), 19: ((0, 1, 0, 4), (0, 2, 0, 2),),
    20: ((0, 1, 1, 4), (0, 1, 2, 4), (0, 2, 1, 2), (0, 2, 2, 2),), 21: ((0, 2, 0, 3),), 25: ((0, 2, 0, 4),), 28: ((1, 0, 0, 0), (1, 0, 2, 0),),
    29: ((1, 0, 1, 0),), 31: ((1, 0, 0, 1),), 32: ((1, 0, 2, 1),), 33: ((0, 2, 2, 3), (1, 0, 1, 1),), 34: ((0, 2, 1, 3), (1, 0, 0, 2),),
    35: ((1, 0, 2, 2),), 36: ((0, 2, 2, 4), (1, 1, 0, 0), (1, 1, 2, 0),), 37: ((0, 2, 1, 4), (1, 0, 1, 2),), 38: ((1, 1, 1, 0),), 39: ((1, 0, 0, 3),),
    40: ((1, 1, 0, 1),), 41: ((1, 1, 2, 1),), 42: ((1, 0, 1, 3), (1, 0, 2, 3), (1, 1, 1, 1),), 43: ((1, 0, 0, 4),),
    44: ((1, 2, 0, 0), (1, 2, 1, 0), (1, 2, 2, 0),), 45: ((1, 0, 1, 4), (1, 0, 2, 4), (1, 1, 0, 2),), 46: ((1, 2, 0, 1),),
    47: ((1, 2, 1, 1), (1, 2, 2, 1),), 48: ((1, 1, 1, 2), (1, 1, 2, 2), (1, 2, 0, 2),), 49: ((1, 2, 1, 2),), 50: ((1, 2, 2, 2),),
    51: ((1, 1, 0, 3), (1, 1, 1, 3), (1, 1, 2, 3), (1, 2, 0, 3),),
    52: ((1, 2, 1, 3), (1, 2, 2, 3), (1, 1, 0, 4), (1, 1, 1, 4), (1, 1, 2, 4), (1, 2, 0, 4), (1, 2, 1, 4), (1, 2, 2, 4),),
}
EPS = 1e-6
VMEM_LIMIT = 67043328


def dot(a, b):
    return lax.dot_general(a, b, (((1,), (0,)), ((), ())), preferred_element_type=F32)


def dot_nt(a, b):
    return lax.dot_general(a, b, (((1,), (1,)), ((), ())), preferred_element_type=F32)


def dot_tn(a, b):
    return lax.dot_general(a, b, (((0,), (0,)), ((), ())), preferred_element_type=F32)


def sigmoid(g):
    return 0.5 * jnp.tanh(0.5 * g) + 0.5


def scale_of(wide):
    return lax.rsqrt(jnp.mean(wide * wide, -1, keepdims=True) + EPS)


def normed(wide):
    return (wide * scale_of(wide)).astype(BF)


def aligned(start, size):
    return pl.ds(pl.multiple_of(start, size), size)


def choose(j, table, do):
    keys = sorted(table)
    if len(keys) == 1:
        pl.when(j == keys[0])(lambda: do(table[keys[0]]))
    elif keys:
        mid = keys[len(keys) // 2]
        pl.when(j < mid)(lambda: choose(j, {k: v for k, v in table.items() if k < mid}, do))
        pl.when(j >= mid)(lambda: choose(j, {k: v for k, v in table.items() if k >= mid}, do))


def kernel(
    n, x_hbm, dy_hbm, gate_hbm, up_hbm, down_hbm, y, fin, dgate_hbm, dup_hbm, ddown_hbm, h_hbm, gu_hbm,
    a1, g, w, acc, act0, act1, g0, g1, terms, slots, io,
    sem, io_sem, gu_sem, first_sem, out_sem, ag_recv, ag_send, side_recv, rs_recv, rs_send, credit,
):
    layers, chunks = w.shape[:2]
    tokens, d = y.shape
    fc = w.shape[-1]
    own = d // n
    half = fc // 2
    tm = tokens // TILES
    big = 2 * tm
    acts, gs = (act0, act1), (g0, g1)
    near = (n - 1) // 2

    me = lax.axis_index("dp")
    core = lax.axis_index("rep") % 2
    left, right = {"dp": (me + n - 1) % n}, {"dp": (me + 1) % n}
    partner = {"rep": lax.axis_index("rep") + 1 - 2 * core}
    owner = [(me + k) % n * own for k in range(n)]

    def remote(src, dst, send, recv, to):
        return pltpu.make_async_remote_copy(src, dst, send, recv, device_id=to, device_id_type=pl.DeviceIdType.MESH)

    ITEMS = [(0, c, m) for c in range(chunks) for m in range(2)] + [(0, slice(None), 2)] + [(l, c, slice(None)) for l in range(1, layers) for c in range(chunks)]

    def piece(i, rows):
        return w.at[(*ITEMS[i], rows, slice(None))]

    def gather(steps):
        for i, h in steps:
            far = near + i % 2
            for side, to in enumerate((right, left)):
                reach = (far, n - 1 - far)[side]
                if h > reach:
                    continue
                ref = piece(i, aligned(owner[(n - h) % n if side == 0 else h] + core * (own // 2), own // 2))
                at = side * far + h
                if h:
                    remote(ref, ref, ag_send.at[i], ag_recv.at[i, at - 1], to).wait_recv()
                if h < reach:
                    remote(ref, ref, ag_send.at[i], ag_recv.at[i, at], to).start()
                if h:
                    remote(ref, ref, ag_send.at[i], side_recv.at[i], partner).start()

    def arrived(*which):
        for i in which:
            ref = piece(i, pl.ds(0, (n - 1) * (own // 2)))
            pltpu.make_async_copy(ref, ref, side_recv.at[i]).wait()

    def reduce(events):
        for turn, p, u, s in events:
            far = near + (p + u) % 2
            for side, to in enumerate((right, left)):
                reach = (far, n - 1 - far)[side]
                if s >= reach:
                    continue
                at = side * far + s
                rows = aligned(owner[reach - s if side == 0 else n - reach + s], own)
                if s == 0:
                    if turn:
                        pl.semaphore_wait(credit.at[side, p, u], 1)
                    ref = terms.at[p, u, rows, :]
                else:
                    ref = slots.at[p, u, at - 1]
                    remote(ref, ref, rs_send.at[p, u], rs_recv.at[p, u, at - 1], to).wait_recv()
                    ref[...] = (ref[...].astype(F32) + terms[p, u, rows, :].astype(F32)).astype(BF)
                remote(ref, slots.at[p, u, at], rs_send.at[p, u], rs_recv.at[p, u, at], to).start()
            if s == near + 1:
                finish(turn, p, u, far)

    def down_out(l, p):
        return pltpu.make_async_copy(fin.at[p, 2], ddown_hbm.at[l - 1, pl.ds(p * own, own), :], out_sem.at[p])

    def in_out(l, m, j):
        out = dgate_hbm if m == 0 else dup_hbm
        return pltpu.make_async_copy(fin.at[j, m], out.at[l - 1, :, pl.ds(j * d, d)], out_sem.at[chunks + m * chunks + j])

    def finish(turn, p, u, far):
        l = layers - 1 - turn
        ends = [slots.at[p, u, far - 1], slots.at[p, u, n - 2]]
        for ref, at in zip(ends, (far - 1, n - 2)):
            remote(ref, ref, rs_send.at[p, u], rs_recv.at[p, u, at], right).wait_recv()
        if turn:
            (down_out(l + 1, p) if u == 2 else in_out(l + 1, u, p)).wait()
        rows = aligned(owner[0], own)
        fin[p, u] = (ends[0][...].astype(F32) + ends[1][...].astype(F32) + terms[p, u, rows, :].astype(F32)).astype(BF)
        ref = w.at[0, 0, 0, pl.ds(0, (n - 1) * own), :]
        pltpu.make_async_copy(ref, ref, rs_send.at[p, u]).wait()
        if l:
            pl.semaphore_signal(credit.at[0, p, u], 1, device_id=left, device_id_type=pl.DeviceIdType.MESH)
            pl.semaphore_signal(credit.at[1, p, u], 1, device_id=right, device_id_type=pl.DeviceIdType.MESH)
        if u == 2 and l:
            down_out(l, p).start()
        if u < 2 and p == chunks - 1:
            low = lax.broadcasted_iota(jnp.int32, (own, 128), 1) < 64
            parts = [[fin[c, u, :, pl.ds(128 * e, 128)] for e in range(fc // 128)] for c in range(chunks)]
            for e in range(fc // 128):
                c0, c1, c2 = (parts[c][e].astype(F32) for c in range(chunks))
                c1 = pltpu.roll(c1, 64, 1)
                for k, (lo, hi) in enumerate(((c0, c1), (c2, c0), (c1, c2))):
                    j, at = divmod(3 * e + k, d // 128)
                    fin[j, u, :, pl.ds(128 * at, 128)] = jnp.where(low, lo, hi).astype(BF)
            for j in range(3) if l else ():
                in_out(l, u, j).start()

    shards = (gate_hbm, up_hbm)
    raw = [
        pltpu.make_async_copy(shards[m].at[l, :, pl.ds(j * d, d)], terms.at[l, m, pl.ds(j * own, own), :], sem.at[2 + (l * 2 + m) * 3 + j])
        for l in range(layers) for m in range(2) for j in range(3)
    ]
    downs = [
        pltpu.make_async_copy(down_hbm.at[l, pl.ds(c * own, own), :], w.at[l, c, 2, aligned(owner[0], own), :], sem.at[2 + layers * 6 + l * 3 + c])
        for l in range(layers) for c in range(chunks)
    ]
    load_x, load_dy = pltpu.make_async_copy(x_hbm, a1, sem.at[0]), pltpu.make_async_copy(dy_hbm, y, sem.at[1])
    for copy in (*raw, *downs, load_x, load_dy):
        copy.start()
    barrier = pltpu.get_barrier_semaphore()
    for to in (left, right, partner):
        pl.semaphore_signal(barrier, 1, device_id=to, device_id_type=pl.DeviceIdType.MESH)
    for copy in (*raw, *downs):
        copy.wait()
    low = lax.broadcasted_iota(jnp.int32, (own, 128), 1) < 64
    for l in range(layers):
        for m in range(2):
            for e in range(fc // 128):
                parts = []
                for k in range(3):
                    j, at = divmod(3 * e + k, d // 128)
                    parts.append(terms[l, m, pl.ds(j * own, own), pl.ds(128 * at, 128)].astype(F32))
                k0, k1, k2 = parts
                mixed = (jnp.where(low, k0, k1), pltpu.roll(jnp.where(low, k2, k0), 64, 1), jnp.where(low, k1, k2))
                for c in range(chunks):
                    w[l, c, m, aligned(owner[0], own), pl.ds(128 * e, 128)] = mixed[c].astype(BF)
    pl.semaphore_wait(barrier, 3)

    gather(GATHER_START[0])
    load_x.wait()

    def norm_x(t, _):
        rows = aligned(t * tm, tm)
        a1[rows, :] = normed(a1[rows, :].astype(F32))
        return 0

    lax.fori_loop(0, TILES, norm_x, 0)
    for steps in GATHER_START[1:]:
        gather(steps)
    arrived(0, 1)

    def hidden_units(keep):
        def keep_out(b):
            return pltpu.make_async_copy(keep.at[b % 3], gu_hbm.at[pl.ds(2 * b, 2)], gu_sem.at[b % 3])

        def body(b, _):
            choose(b, GATHER_HIDDEN, gather)
            choose(b, {BODIES * c: (2 * c, 2 * c + 1) for c in range(1, chunks)}, lambda which: arrived(*which))
            pl.when(b >= 3)(lambda: keep_out(b - 3).wait())
            c = b // BODIES
            for k in range(2):
                rows = aligned(b % BODIES * big + k * tm, tm)
                at = a1[rows, :]
                for f in (0, half):
                    gate = dot(at, w[0, c, 0, :, f : f + half])
                    up = dot(at, w[0, c, 1, :, f : f + half])
                    keep[b % 3, k, 0, :, f : f + half] = gate
                    keep[b % 3, k, 1, :, f : f + half] = up
                    g[c, rows, f : f + half] = (gate * sigmoid(gate) * up).astype(BF)
            keep_out(b).start()
            return 0

        lax.fori_loop(0, chunks * BODIES, body, 0)
        for b in range(chunks * BODIES - 3, chunks * BODIES):
            keep_out(b).wait()

    def io_in(src, j):
        return pltpu.make_async_copy(src.at[aligned(j * big, big), :], io.at[j % 2], io_sem.at[0, j % 2])

    io_in(x_hbm, 0).start()
    io_in(x_hbm, 1).start()
    pl.run_scoped(hidden_units, pltpu.VMEM((3, 2, 2, tm, fc), F32))

    def backward(turn, a, gate_up, start, pending):
        l = layers - 1 - turn
        width = WIDTHS[turn]
        bodies = TILES // width
        table = {at - start: steps for at, steps in SUMS.items() if at >= start}
        loop = chunks * bodies
        tiles = chunks * TILES

        def grads_in(i, slot, f, kept):
            c, t = i // TILES, i % TILES
            rows = aligned(t * tm, tm)
            if kept is None:
                at = a[rows, :]
                gate = dot(at, w[l, c, 0, :, f : f + half])
                up = dot(at, w[l, c, 1, :, f : f + half])
            else:
                gate, up = kept[0, :, f : f + half], kept[1, :, f : f + half]
            dact = dot_nt(y[rows, :], w[l, c, 2, f : f + half, :]).astype(BF).astype(F32)
            s = sigmoid(gate)
            silu = gate * s
            acts[slot][:, f : f + half] = (silu * up).astype(BF)
            dgate = (dact * up * (s + silu * (1.0 - s))).astype(BF)
            dup = (dact * silu).astype(BF)
            gs[slot][:, f : f + half] = dgate
            gs[slot][:, fc + f : fc + f + half] = dup
            g[c, rows, f : f + half] = dgate
            g[c, rows, fc + f : fc + f + half] = dup

        def down_grad(i, slot):
            rows = aligned(i % TILES * tm, tm)
            acc[2] += dot_tn(acts[slot][...], y[rows, :])

        def in_grad(i, slot, m):
            rows = aligned(i % TILES * tm, tm)
            acc[m] += dot_tn(a[rows, :], gs[slot][:, m * fc : (m + 1) * fc])

        def first_of(j):
            return jnp.minimum(2 * j + 1, tiles - 2)

        def block_in(j):
            return pltpu.make_async_copy(gu_hbm.at[pl.ds(first_of(j), 2)], gate_up.at[j % 3], gu_sem.at[j % 3])

        src = h_hbm if l else x_hbm
        io_in(src, 0).start()
        io_in(src, 1).start()
        if turn:
            block_in(1).start()
            for copy in first_tiles:
                copy.wait()
            for k in range(2):
                for m in range(2):
                    gate_up[0, k, m] = acc[1 + k, pl.ds(m * tm, tm), :]
        for f in (0, half):
            grads_in(0, 0, f, acc.at[0].reshape(2, tm, fc) if turn else None)
        if turn:
            for m in range(3):
                acc[m] = jnp.zeros_like(acc[m])

        def body(j, _):
            if not turn:
                choose(j, GATHER_BACK, gather)
                choose(j, {bodies * c - 1: 3 * chunks - 2 + c for c in range(1, chunks)}, lambda i: arrived(i))
            choose(j, {at: steps for at, steps in table.items() if at < loop}, reduce)
            if turn:
                pl.when(j > 0)(lambda: block_in(j).wait())
                pl.when(j + 2 < loop)(lambda: block_in(j + 2).start())
            for k in range(width):
                i = width * j + k
                ahead = jnp.minimum(i + 1, tiles - 1)
                kept = gate_up.at[j % 3, ahead - first_of(j) if k == 0 else 1] if turn else None
                parts = [
                    functools.partial(grads_in, ahead, (k + 1) % 2, 0, kept),
                    functools.partial(down_grad, i, k % 2),
                    functools.partial(in_grad, i, k % 2, 0),
                    functools.partial(grads_in, ahead, (k + 1) % 2, half, kept),
                    functools.partial(in_grad, i, k % 2, 1),
                ]
                for part in ORDERS[turn]:
                    parts[part]()
            return 0

        def chunk(c, _):
            lax.fori_loop(c * bodies, (c + 1) * bodies, body, 0)
            for m in range(3):
                terms[c, m] = acc[m].astype(BF)
                acc[m] = jnp.zeros_like(acc[m])
            return 0

        lax.fori_loop(0, chunks, chunk, 0)
        for copy in pending:
            copy.wait()
        for copy in first_tiles if not turn else ():
            copy.start()

        def inputs(j, _):
            choose(j, {at - loop: steps for at, steps in table.items() if loop <= at < loop + BODIES}, reduce)
            io_in(src, j).wait()
            for k in range(2):
                rows = aligned(j * big + k * tm, tm)
                da = sum(dot_nt(g[c, rows, m * fc : (m + 1) * fc], w[l, c, m]) for c in range(chunks) for m in range(2))
                da = da.astype(BF).astype(F32)
                wide = io[j % 2, pl.ds(k * tm, tm), :].astype(F32)
                scale = scale_of(wide)
                along = jnp.mean(da * wide, -1, keepdims=True) * (scale * scale * scale)
                dh = (da * scale - wide * along).astype(BF).astype(F32)
                y[rows, :] = (y[rows, :].astype(F32) + dh).astype(BF)
            pl.when(j + 2 < BODIES)(lambda: io_in(src, j + 2).start())
            return 0

        lax.fori_loop(0, BODIES, inputs, 0)

    for m in range(3):
        acc[m] = jnp.zeros_like(acc[m])
    first_tiles = [pltpu.make_async_copy(gu_hbm.at[k, m], acc.at[k, pl.ds(m * tm, tm), :], first_sem.at[k, m]) for k in range(3) for m in range(2)]

    def with_last(a2, out):
        def io_out(j):
            return pltpu.make_async_copy(out.at[j % 2], h_hbm.at[aligned(j * big, big), :], io_sem.at[1, j % 2])

        def down(j, _):
            choose(j, GATHER_DOWN, gather)
            pl.when(j == 0)(lambda: arrived(2 * chunks))
            io_in(x_hbm, j).wait()
            pl.when(j >= 2)(lambda: io_out(j - 2).wait())
            for k in range(4):
                rows = aligned(j * big + k * (tm // 2), tm // 2)
                hidden = sum(dot(g[c, rows, :fc], w[0, c, 2]) for c in range(chunks))
                here = pl.ds(k * (tm // 2), tm // 2)
                h = (io[j % 2, here, :].astype(F32) + hidden.astype(BF).astype(F32)).astype(BF)
                out[j % 2, here, :] = h
                a2[rows, :] = normed(h.astype(F32))
            io_out(j).start()
            pl.when(j + 2 < BODIES)(lambda: io_in(x_hbm, j + 2).start())
            return 0

        lax.fori_loop(0, BODIES, down, 0)
        load_dy.wait()
        arrived(2 * chunks + 1)
        backward(0, a2, None, 0, [io_out(BODIES - 2), io_out(BODIES - 1)])

    pl.run_scoped(with_last, pltpu.VMEM((tokens, d), BF), pltpu.VMEM((2, big, d), BF))

    def with_first(gate_up):
        backward(1, a1, gate_up, chunks * TILES // WIDTHS[0] + BODIES, ())

    pl.run_scoped(with_first, pltpu.VMEM((3, 2, 2, tm, fc), F32))

    reduce(SUMS[max(SUMS)])
    for i in range(len(ITEMS)):
        ref = piece(i, pl.ds(0, (n - 1) * own))
        pltpu.make_async_copy(ref, ref, ag_send.at[i]).wait()


def layers_of(n, x, dy, gate, up, down):
    tokens, d = x.shape
    layers, own, ff = gate.shape
    fc = ff // CHUNKS
    tm = tokens // TILES
    items = 3 * CHUNKS + 1
    assert d == fc == n * own and down.shape == (layers, CHUNKS * own, d) and own == 64
    assert n == 8 and layers == 2
    hbm, vmem = pl.BlockSpec(memory_space=pl.ANY), pl.BlockSpec(memory_space=pltpu.VMEM)
    dma = pltpu.SemaphoreType.DMA
    kept = jax.ShapeDtypeStruct((CHUNKS * TILES, 2, tm, fc), F32)
    return pl.pallas_call(
        functools.partial(kernel, n),
        out_shape=[
            pltpu.VMEM((tokens, d), BF),
            pltpu.VMEM((CHUNKS, 3, own, fc), BF),
            *(jax.ShapeDtypeStruct((layers - 1, *t.shape[1:]), BF) for t in (gate, up, down)),
            jax.ShapeDtypeStruct(x.shape, BF),
            kept,
        ],
        in_specs=[hbm] * 5,
        out_specs=[vmem] * 2 + [hbm] * 5,
        scratch_shapes=[
            pltpu.VMEM((tokens, d), BF),
            pltpu.VMEM((CHUNKS, tokens, 2 * fc), BF),
            pltpu.VMEM((layers, CHUNKS, 3, d, fc), BF),
            pltpu.VMEM((3, d, fc), F32),
            pltpu.VMEM((tm, fc), BF),
            pltpu.VMEM((tm, fc), BF),
            pltpu.VMEM((tm, 2 * fc), BF),
            pltpu.VMEM((tm, 2 * fc), BF),
            pltpu.VMEM((CHUNKS, 3, d, fc), BF),
            pltpu.VMEM((CHUNKS, 3, n - 1, own, fc), BF),
            pltpu.VMEM((2, 2 * tm, d), BF),
            dma((2 + layers * 9,)),
            dma((2, 2)),
            dma((3,)),
            dma((3, 2)),
            dma((CHUNKS * 3,)),
            dma((items, n - 1)),
            dma((items,)),
            dma((items,)),
            dma((CHUNKS, 3, n - 1)),
            dma((CHUNKS, 3)),
            pltpu.SemaphoreType.REGULAR((2, CHUNKS, 3)),
        ],
        compiler_params=pltpu.CompilerParams(vmem_limit_bytes=VMEM_LIMIT - (tokens * d + CHUNKS * 3 * own * fc) * 2, has_side_effects=True, collective_id=0),
        name="layers",
    )(x, dy, gate, up, down)[:5]


def outputs(layers, dx, first, *others):
    tokens, d = dx.shape
    chunks, _, own, fc = first.shape
    wide, tall = (layers, own, chunks * fc), (layers, chunks * own, d)

    def kernel(dx_ref, first_ref, gate_in, up_in, down_in, dx_out, gate_out, up_out, down_out, *rest):
        *bufs, sem, in_sem = rest
        grads = (gate_out, up_out, down_out)
        ins = [pltpu.make_async_copy(s, buf, in_sem.at[k]) for k, (s, buf) in enumerate(zip((gate_in, up_in, down_in), bufs))]
        moves = [pltpu.make_async_copy(dx_ref, dx_out, sem.at[0])]
        for m, out in enumerate(grads):
            for j in range(chunks):
                place = out.at[0, :, pl.ds(j * fc, fc)] if m < 2 else out.at[0, pl.ds(j * own, own), :]
                moves.append(pltpu.make_async_copy(first_ref.at[j, m], place, sem.at[1 + m * chunks + j]))
        for copy in (*ins, *moves):
            copy.start()
        for k, (copy, buf, out) in enumerate(zip(ins, bufs, grads)):
            copy.wait()
            moves.append(pltpu.make_async_copy(buf, out.at[pl.ds(1, layers - 1)], sem.at[1 + 3 * chunks + k]))
            moves[-1].start()
        for copy in moves:
            copy.wait()

    hbm, vmem = pl.BlockSpec(memory_space=pl.ANY), pl.BlockSpec(memory_space=pltpu.VMEM)
    kept = [pltpu.with_memory_space_constraint(t, pltpu.VMEM) for t in (dx, first)]
    return pl.pallas_call(
        kernel,
        out_shape=[jax.ShapeDtypeStruct(s, BF) for s in ((tokens, d), wide, wide, tall)],
        in_specs=[vmem] * 2 + [hbm] * 3,
        out_specs=[hbm] * 4,
        scratch_shapes=[*(pltpu.VMEM(t.shape, BF) for t in others), pltpu.SemaphoreType.DMA((4 + 3 * chunks,)), pltpu.SemaphoreType.DMA((3,))],
        compiler_params=pltpu.CompilerParams(vmem_limit_bytes=VMEM_LIMIT - (dx.size + first.size) * 2),
        name="outputs",
    )(*kept, *others)


def solution(mesh):
    n = mesh.shape["dp"]
    assert mesh.shape["rep"] % 2 == 0

    def local(x, dy, gate, up, down):
        dx, *grads = outputs(gate.shape[0], *layers_of(n, x[0], dy[0], gate, up, down))
        return dx[None], *grads

    both, rows = P(("rep", "dp"), None, None), P(None, "dp", None)
    grads = P("rep", "dp", None)
    return jax.shard_map(
        local, mesh=mesh, in_specs=(both, both, rows, rows, rows), out_specs=(both, grads, grads, grads), check_vma=False
    )
```
